512 devices in a mesh: lon: 64 (over y, z_hi, core), lat: 8 (over z_lo, x).
Axes of the slice: x: 4, y: 8, z: 8 (z_hi: 4, z_lo: 2; z = z_hi * 2 + z_lo), core: 2. Of those that a mesh axis runs over, the one named last changes fastest.
Arguments:
- target: float32 [3, 128, 65536], P(None, 'lat', 'lon'), may hold values from -6 to 6
- grad_x: float32 [2, 3, 128, 65536], P(None, None, 'lat', 'lon'), may hold values from -6 to 6
- grad_y: float32 [2, 3, 128, 65536], P(None, None, 'lat', 'lon'), may hold values from -6 to 6
- labels: int32 [128, 65536], P('lat', 'lon'), may hold values from 0 to 1
- sweeps: int32 [3], replicated, may hold values from 2 to 4
Outputs:
- stitched: float32 [3, 128, 65536], P(None, 'lat', 'lon')
The draws below stay inside these ranges and needn't reach their ends.
All inputs are finite; a program needn't handle non-finite values.
Results may differ from the reference program's by a relative error of at most 0.0004.
Values sent between devices are 32-bit elements; how exact they have to be, the bound alone decides.
A program may use at most 64 MiB of HBM per device.

```python
import jax
import jax.numpy as jnp
from jax import lax

SOURCES = 2
LEVELS = 3
MAXS = 4
NY = 128
NX = 65536


def gradient_field(key):
    noise_key = jax.random.fold_in(key, 0)
    shape = (SOURCES, 3, NY, NX)
    return jnp.clip(0.5 * jax.random.normal(noise_key, shape, jnp.float32), -6.0, 6.0)


def draw_grad_x(key, part):
    return gradient_field(jax.random.fold_in(key, 101))


def draw_grad_y(key, part):
    return gradient_field(jax.random.fold_in(key, 202))


def plant(entries, key, least, top_value):
    place = [jax.random.randint(jax.random.fold_in(key, axis), (), 0, length) for axis, length in enumerate(entries.shape)]
    longest = entries.shape.index(max(entries.shape))
    neighbour = place[:longest] + [(place[longest] + 1) % entries.shape[longest]] + place[longest + 1:]
    return entries.at[tuple(place)].set(least).at[tuple(neighbour)].set(top_value)


def block_scale(rng, dims, cuts, low, top_value):
    factor_of, own = 1.0, jax.random.fold_in(rng, 6)
    for dim, shards_of in cuts:
        draws = jnp.exp(jax.random.uniform(jax.random.fold_in(own, dim), (shards_of,), jnp.float32, low / len(cuts), top_value / len(cuts)))
        factor_of = factor_of * jnp.repeat(draws, dims[dim] // shards_of).reshape([-1 if axis == dim else 1 for axis in range(len(dims))])
    return factor_of


def centred(key, shape, scale, most, shards=(), held_as=jnp.bfloat16):
    values = jax.random.normal(key, shape, jnp.float32) * scale
    if len(shards) > 0:
        values = block_scale(key, shape, shards, -0.22, 0.18) * values
    return jnp.clip(values, min=-most, max=most).astype(held_as)


def setup_inputs(seed: int = 0) -> dict:
    key_of = jax.random.split(jax.random.key(seed), 6)
    return {
        "target": centred(key_of[0], (3, NY, NX), 1.0, 6.0, ((1, 8), (2, 64)), jnp.float32),
        "grad_x": draw_grad_x(jax.random.fold_in(key_of[5], 71), 0),
        "grad_y": draw_grad_y(jax.random.fold_in(key_of[5], 71), 0),
        "labels": plant(jax.random.randint(key_of[3], (NY, NX), 0, SOURCES), jax.random.fold_in(key_of[3], 1), 0, SOURCES - 1).astype(jnp.int32),
        "sweeps": jax.random.randint(key_of[4], (LEVELS,), 2, MAXS + 1).astype(jnp.int32),
    }


screening = 0.02
damping = 0.8


def wrap_pad(field, width):
    field = jnp.concatenate([field[:, :, -width:], field, field[:, :, :width]], axis=2)
    return jnp.pad(field, ((0, 0), (width, width), (0, 0)))


def stencil(padded, scale):
    inner = padded[:, 1:-1, 1:-1]
    beside = padded[:, :-2, 1:-1] + padded[:, 2:, 1:-1] + padded[:, 1:-1, :-2] + padded[:, 1:-1, 2:]
    return (screening + 4.0 * scale) * inner - scale * beside


def smooth(field, right, count, scale):
    diag = screening + 4.0 * scale

    def sweep(step, value):
        return value + damping * (right - stencil(wrap_pad(value, 1), scale)) / diag

    return lax.fori_loop(0, count, sweep, field)


def restrict(field):
    chans, rows, cols = field.shape
    return field.reshape(chans, rows // 2, 2, cols // 2, 2).mean(axis=(2, 4))


def prolong_from(padded):
    center = padded[:, 1:-1, 1:-1]
    north = padded[:, :-2, 1:-1]
    south = padded[:, 2:, 1:-1]
    west = padded[:, 1:-1, :-2]
    east = padded[:, 1:-1, 2:]
    f00 = 0.5625 * center + 0.1875 * north + 0.1875 * west + 0.0625 * padded[:, :-2, :-2]
    f01 = 0.5625 * center + 0.1875 * north + 0.1875 * east + 0.0625 * padded[:, :-2, 2:]
    f10 = 0.5625 * center + 0.1875 * south + 0.1875 * west + 0.0625 * padded[:, 2:, :-2]
    f11 = 0.5625 * center + 0.1875 * south + 0.1875 * east + 0.0625 * padded[:, 2:, 2:]
    stacked = jnp.stack([jnp.stack([f00, f01], -1), jnp.stack([f10, f11], -1)], 2)
    chans, rows, two, cols, other = stacked.shape
    return stacked.reshape(chans, rows * 2, cols * 2)


def cycle(level, field, right, sweeps):
    scale = 0.25 ** level
    count = sweeps[level]
    field = smooth(field, right, count, scale)
    if level + 1 == LEVELS:
        return field
    resid = right - stencil(wrap_pad(field, 1), scale)
    coarse = restrict(resid)
    fix = cycle(level + 1, jnp.zeros_like(coarse), coarse, sweeps)
    field = field + prolong_from(wrap_pad(fix, 1))
    return smooth(field, right, count, scale)


def reference(target, grad_x, grad_y, labels, sweeps):
    sel_x = jnp.zeros_like(target)
    sel_y = jnp.zeros_like(target)
    for source in range(SOURCES):
        picked = (labels == source)[None, :, :]
        sel_x = jnp.where(picked, grad_x[source], sel_x)
        sel_y = jnp.where(picked, grad_y[source], sel_y)
    west = jnp.roll(sel_x, 1, axis=2)
    north = jnp.concatenate([jnp.zeros_like(sel_y[:, :1, :]), sel_y[:, :-1, :]], axis=1)
    right = screening * target - ((sel_x - west) + (sel_y - north))
    return cycle(0, target, right, sweeps)
```

```python
import functools

import jax
import jax.numpy as jnp
from jax import lax
from jax.experimental import pallas as pl
from jax.experimental.pallas import tpu as pltpu
from jax.sharding import PartitionSpec as P

SOURCES = 2
LEVELS = 3
MAXS = 4
CH = 3
ROWS = 16
TILES = 8
L = 128

screening = 0.02
damping = 0.8
MESH = pl.DeviceIdType.MESH

T0, T1, T2 = TILES + 1, TILES // 2 + 1, TILES // 4 + 1
R0 = 24
R1 = 56
R2 = 24
RP = 24


def iota(rows, dim):
    return lax.broadcasted_iota(jnp.int32, (rows, L), dim)


def lanes_of(rows):
    lane = iota(rows, 1)
    return lane == 0, lane == L - 1, lane < L // 2


def up(x):
    return pltpu.roll(x, x.shape[0] - 1, 0)


def down(x):
    return pltpu.roll(x, 1, 0)


def left(x):
    return pltpu.roll(x, L - 1, 1)


def right(x):
    return pltpu.roll(x, 1, 1)


def beside(xs, first, last):
    rights = [right(x) for x in xs]
    lefts = [left(x) for x in xs]
    count = len(xs)
    sums = []
    for t, x in enumerate(xs):
        west = jnp.where(first, rights[t - 1], rights[t])
        east = jnp.where(last, lefts[(t + 1) % count], lefts[t])
        sums.append((up(x) + down(x)) + (west + east))
    return sums


def sweep(src, dst, rhs, tiles, rows, base, factor, scale):
    diag = screening + 4.0 * scale
    first, last, _ = lanes_of(rows)

    def body(c, carry):
        xs = [src[c, t] for t in range(tiles)]
        sums = beside(xs, first, last)
        for t in range(tiles):
            b = rhs[c, t, base : base + rows]
            dst[c, t] = xs[t] + factor * ((b - diag * xs[t]) + scale * sums[t])
        return carry

    lax.fori_loop(0, CH, body, 0)


def restrict(src, rhs, dst, dst_base, tmp, tiles, rows, start, count, scale):
    diag = screening + 4.0 * scale
    first, last, _ = lanes_of(rows)
    low = lanes_of(count)[2]
    pick = (2 * iota(count, 1)) % L

    def body(c, carry):
        xs = [src[c, t] for t in range(tiles)]
        sums = beside(xs, first, last)
        for t in range(tiles):
            tmp[t, 0:rows] = (rhs[c, t, 0:rows] - diag * xs[t]) + scale * sums[t]
        parts = []
        for t in range(tiles):
            pair = tmp[t, pl.ds(start, count, stride=2)] + tmp[t, pl.ds(start + 1, count, stride=2)]
            pair = pair + left(pair)
            parts.append(0.25 * jnp.take_along_axis(pair, pick, axis=1))
        for t in range(tiles // 2):
            dst[c, t, dst_base : dst_base + count] = jnp.where(low, parts[2 * t], parts[2 * t + 1])
        dst[c, tiles // 2, dst_base : dst_base + count] = parts[-1]
        return carry

    lax.fori_loop(0, CH, body, 0)


def prolong_rows(src, c, tiles, rows, tmp):
    for t in range(tiles):
        x = src[c, t]
        tmp[t, pl.ds(0, rows, stride=2)] = 0.75 * x + 0.25 * down(x)
        tmp[t, pl.ds(1, rows, stride=2)] = 0.75 * x + 0.25 * up(x)


def prolong_cols(xs, rows):
    lane = iota(rows, 1)
    first, last, low = lanes_of(rows)
    aside = jnp.where(lane % 2 == 0, L - 1, 1)
    count = len(xs)
    out = []
    for t in range(count):
        wests = right(xs[t - 1])
        easts = left(xs[(t + 1) % count])
        for h in range(2 if t < count - 1 else 1):
            here = lane // 2 + (h * (L // 2) if t < count - 1 else jnp.where(low, 0, L // 2))
            near = jnp.take_along_axis(xs[t], here, axis=1)
            far = jnp.take_along_axis(xs[t], (here + aside) % L, axis=1)
            if h == 0:
                far = jnp.where(first, wests, far)
            if h == 1 or t == count - 1:
                far = jnp.where(last, easts, far)
            out.append(0.75 * near + 0.25 * far)
    return out


def kernel(
    sweeps, target, grad_x, grad_y, labels, out,
    gx, gy, lab, v0, w0, b0, sx, wx, sy, ny, ps, pn, rn, rs, re, rw,
    b1, v1, w1, vp, wp, b2, v2, w2, zn, zs, tmp,
    in_sem, send, recv,
):
    lon, lat = lax.axis_index("lon"), lax.axis_index("lat")
    nlon, nlat = lax.axis_size("lon"), lax.axis_size("lat")

    def peer(dlat, dlon):
        return {"lat": lax.rem(lat + dlat + nlat, nlat), "lon": lax.rem(lon + dlon + nlon, nlon)}

    loads = [
        pltpu.make_async_copy(labels, lab, in_sem.at[0]),
        pltpu.make_async_copy(grad_x, gx, in_sem.at[1]),
        pltpu.make_async_copy(grad_y, gy, in_sem.at[2]),
    ]
    for t in range(TILES):
        loads.append(
            pltpu.make_async_copy(
                target.at[:, :, pl.ds(t * L, L)], v0.at[:, t, pl.ds(0, ROWS)], in_sem.at[3 + t]
            )
        )
    for load in loads:
        load.start()

    peers = [(d, 0) for d in (1, -1, 2, -2, 3, -3)]
    peers += [(i, j) for i in (-1, 0, 1) for j in (-1, 1)]
    barrier = pltpu.get_barrier_semaphore()
    for dlat, dlon in peers:
        pl.semaphore_signal(barrier, inc=1, device_id=peer(dlat, dlon), device_id_type=MESH)

    used = [0]

    def remote(src, dst, dlat, dlon):
        k = used[0]
        used[0] += 1
        return pltpu.make_async_remote_copy(
            src_ref=src,
            dst_ref=dst,
            send_sem=send.at[k],
            recv_sem=recv.at[k],
            device_id=peer(dlat, dlon),
            device_id_type=MESH,
        )

    first, last, low = lanes_of(ROWS)
    first8, last8, low8 = lanes_of(8)
    sub8 = iota(8, 0)
    north_half = sub8 < 4
    row16 = iota(ROWS, 0)

    def factors(level, rows, total, at):
        diag = screening + 4.0 * 0.25**level
        here = iota(rows, 0)
        here = at(here) + lat * (ROWS >> level)
        inside = jnp.where((here >= 0) & (here < total), 1.0, 0.0).astype(jnp.float32)
        steps = [
            jnp.where(sweeps[level] > i, damping / diag, 0.0).astype(jnp.float32) for i in range(MAXS)
        ]
        return inside, [inside * step for step in steps]

    for load in loads[:3]:
        load.wait()

    def picked(ref, c, t, rows):
        cols = slice(t * L, (t + 1) * L)
        return jnp.where(lab[rows, cols] == 0, ref[0, c, rows, cols], ref[1, c, rows, cols])

    for c in range(CH):
        sx[c] = picked(gx, c, TILES - 1, slice(0, ROWS))
    for t in range(TILES):
        edge = [pltpu.roll(picked(gy, c, t, slice(8, 16)), c + 1, 0) for c in range(CH)]
        sy[t] = jnp.where(sub8 == 0, edge[0], jnp.where(sub8 == 1, edge[1], edge[2]))

    pl.semaphore_wait(barrier, len(peers))
    to_south = remote(sy, ny, 1, 0)
    to_east = remote(sx, wx, 0, 1)
    to_south.start()
    to_east.start()

    for load in loads[3:]:
        load.wait()
    t_east = remote(v0.at[:, TILES - 1, pl.ds(0, ROWS)], rw.at[0], 0, 1)
    t_west = remote(v0.at[:, 0, pl.ds(0, ROWS)], re.at[0], 0, -1)
    t_east.start()
    t_west.start()

    def rhs_body(c, carry):
        before = None
        for t in range(TILES):
            x = picked(gx, c, t, slice(0, ROWS))
            y = picked(gy, c, t, slice(0, ROWS))
            moved = right(x)
            west = jnp.where(first, 0.0 if t == 0 else before, moved)
            before = moved
            north = jnp.where(row16 == 0, 0.0, down(y))
            b0[c, t, 0:ROWS] = screening * v0[c, t, 0:ROWS] - ((x - west) + (y - north))
        return carry

    lax.fori_loop(0, CH, rhs_body, 0)

    to_south.wait()
    to_east.wait()
    has_north = jnp.where(lat > 0, 1.0, 0.0).astype(jnp.float32)
    for c in range(CH):
        b0[c, 0, 0:ROWS] = b0[c, 0, 0:ROWS] + jnp.where(first, right(wx[c]), 0.0)
        for t in range(TILES):
            row = pltpu.roll(ny[t], 8 - c, 0) if c else ny[t]
            b0[c, t, 0:8] = b0[c, t, 0:8] + jnp.where(sub8 == 0, row * has_north, 0.0)

    def pack_body(c, carry):
        for t in range(TILES):
            v, b = v0[c, t, 8:16], b0[c, t, 8:16]
            b = b + jnp.where(sub8 == 4, down(v), 0.0)
            ps[c, t] = jnp.where(north_half, pltpu.roll(b, 4, 0), v)
            v, b = v0[c, t, 0:8], b0[c, t, 0:8]
            b = b + jnp.where(sub8 == 3, up(v), 0.0)
            pn[c, t] = jnp.where(north_half, v, pltpu.roll(b, 4, 0))
        return carry

    lax.fori_loop(0, CH, pack_body, 0)

    e0 = [
        remote(ps, rn.at[:, pl.ds(0, TILES)], 1, 0),
        remote(pn, rs.at[:, pl.ds(0, TILES)], -1, 0),
        remote(ps.at[:, TILES - 1], rn.at[:, TILES + 1], 1, 1),
        remote(ps.at[:, 0], rn.at[:, TILES], 1, -1),
        remote(pn.at[:, TILES - 1], rs.at[:, TILES + 1], -1, 1),
        remote(pn.at[:, 0], rs.at[:, TILES], -1, -1),
        remote(b0.at[:, TILES - 1, pl.ds(0, ROWS)], rw.at[1], 0, 1),
        remote(b0.at[:, 0, pl.ds(0, ROWS)], re.at[1], 0, -1),
    ]
    for copy in e0:
        copy.start()

    inside0, f0 = factors(0, R0, nlat * ROWS, lambda i: jnp.where(i < 20, i, i - 24))
    inside1, f1 = factors(1, R1, nlat * ROWS // 2, lambda i: i - 24)
    inside2, f2 = factors(2, R2, nlat * ROWS // 4, lambda i: i - 8)
    insidep, fp = factors(1, RP, nlat * ROWS // 2, lambda i: i - 8)

    for copy in e0:
        copy.wait()
    t_east.wait()
    t_west.wait()

    in8 = inside0[16:24]

    def halo(south, north):
        v = jnp.where(north_half, south, north) * in8
        b = pltpu.roll(jnp.where(north_half, north, south), 4, 0)
        b = b - jnp.where(sub8 == 3, up(v), jnp.where(sub8 == 4, down(v), 0.0))
        return v, b

    def fill_body(c, carry):
        for t in range(TILES):
            v, b = halo(rs[c, t], rn[c, t])
            v0[c, t, 16:24] = v
            b0[c, t, 16:24] = b
        v, b = halo(
            jnp.where(low8, rs[c, TILES], rs[c, TILES + 1]), jnp.where(low8, rn[c, TILES], rn[c, TILES + 1])
        )
        v0[c, TILES, 16:24] = v
        b0[c, TILES, 16:24] = b
        v0[c, TILES, 0:ROWS] = jnp.where(low, re[0, c], rw[0, c])
        b0[c, TILES, 0:ROWS] = jnp.where(low, re[1, c], rw[1, c])
        return carry

    lax.fori_loop(0, CH, fill_body, 0)

    for i in range(MAXS):
        a, b = (v0, w0) if i % 2 == 0 else (w0, v0)
        sweep(a, b, b0, T0, R0, 0, f0[i], 1.0)

    own = pl.ds(24, 8)
    restrict(v0, b0, b1, 24, tmp, T0, R0, 0, 8, 1.0)
    e1 = [remote(b1.at[:, :, own], b1.at[:, :, pl.ds(24 - 8 * d, 8)], d, 0) for d in (2, -2, 1, -1, 3, -3)]
    e2 = [remote(v0.at[:, :, pl.ds(0, 8)], zs, -1, 0), remote(v0.at[:, :, pl.ds(8, 8)], zn, 1, 0)]
    for copy in e1 + e2:
        copy.start()
    for copy in e1:
        copy.wait()

    def first1(c, carry):
        for t in range(T1):
            v1[c, t] = f1[0] * b1[c, t]
        return carry

    lax.fori_loop(0, CH, first1, 0)
    sweep(v1, w1, b1, T1, R1, 0, f1[1], 0.25)
    sweep(w1, v1, b1, T1, R1, 0, f1[2], 0.25)
    sweep(v1, w1, b1, T1, R1, 0, f1[3], 0.25)
    restrict(w1, b1, b2, 0, tmp, T1, R1, 8, R2, 0.25)

    def first2(c, carry):
        for t in range(T2):
            v2[c, t] = f2[0] * b2[c, t]
        return carry

    lax.fori_loop(0, CH, first2, 0)
    sweep(v2, w2, b2, T2, R2, 0, f2[1], 0.0625)
    sweep(w2, v2, b2, T2, R2, 0, f2[2], 0.0625)
    sweep(v2, w2, b2, T2, R2, 0, f2[3], 0.0625)

    def up1(c, carry):
        prolong_rows(w2, c, T2, R2, tmp)
        fine = prolong_cols([tmp[t, 8:32] for t in range(T2)], RP)
        for t in range(T1):
            vp[c, t] = (w1[c, t, 16:40] + fine[t]) * insidep
        return carry

    lax.fori_loop(0, CH, up1, 0)
    for i in range(MAXS):
        a, b = (vp, wp) if i % 2 == 0 else (wp, vp)
        sweep(a, b, b1, T1, RP, 16, fp[i], 0.25)

    for copy in e2:
        copy.wait()

    def up0(c, carry):
        prolong_rows(vp, c, T1, RP, tmp)
        ends = [jnp.where(north_half, tmp[t, 32:40], tmp[t, 8:16]) for t in range(T1)]
        mids = prolong_cols([tmp[t, 16:32] for t in range(T1)], ROWS)
        ends = prolong_cols(ends, 8)
        for t in range(T0):
            v0[c, t, 0:ROWS] = v0[c, t, 0:ROWS] + mids[t]
            v0[c, t, 16:24] = (jnp.where(north_half, zs[c, t], zn[c, t]) + ends[t]) * in8
        return carry

    lax.fori_loop(0, CH, up0, 0)
    for i in range(MAXS):
        a, b = (v0, w0) if i % 2 == 0 else (w0, v0)
        sweep(a, b, b0, T0, R0, 0, f0[i], 1.0)
    for c in range(CH):
        for t in range(TILES):
            out[c, :, t * L : (t + 1) * L] = v0[c, t, 0:ROWS]


def local(target, grad_x, grad_y, labels, sweeps):
    f32 = jnp.float32

    def vmem(*shape):
        return pltpu.VMEM(shape + (L,), f32)

    scratch = [
        pltpu.VMEM(grad_x.shape, f32),
        pltpu.VMEM(grad_y.shape, f32),
        pltpu.VMEM(labels.shape, jnp.int32),
        vmem(CH, T0, R0), vmem(CH, T0, R0), vmem(CH, T0, R0),
        vmem(CH, ROWS), vmem(CH, ROWS),
        vmem(TILES, 8), vmem(TILES, 8),
        vmem(CH, TILES, 8), vmem(CH, TILES, 8),
        vmem(CH, TILES + 2, 8), vmem(CH, TILES + 2, 8),
        vmem(2, CH, ROWS), vmem(2, CH, ROWS),
        vmem(CH, T1, R1), vmem(CH, T1, R1), vmem(CH, T1, R1),
        vmem(CH, T1, RP), vmem(CH, T1, RP),
        vmem(CH, T2, R2), vmem(CH, T2, R2), vmem(CH, T2, R2),
        vmem(CH, T0, 8), vmem(CH, T0, 8),
        vmem(T0, R1),
        pltpu.SemaphoreType.DMA((3 + TILES,)),
        pltpu.SemaphoreType.DMA((20,)),
        pltpu.SemaphoreType.DMA((20,)),
    ]
    anywhere = pl.BlockSpec(memory_space=pl.ANY)
    return pl.pallas_call(
        kernel,
        out_shape=jax.ShapeDtypeStruct(target.shape, f32),
        in_specs=[pl.BlockSpec(memory_space=pltpu.SMEM)] + [anywhere] * 4,
        out_specs=pl.BlockSpec(memory_space=pltpu.VMEM),
        scratch_shapes=scratch,
        compiler_params=pltpu.CompilerParams(collective_id=0, has_side_effects=True),
        name="vcycle",
    )(sweeps, target, grad_x, grad_y, labels)


def solution(mesh):
    in_specs = (
        P(None, "lat", "lon"),
        P(None, None, "lat", "lon"),
        P(None, None, "lat", "lon"),
        P("lat", "lon"),
        P(),
    )
    out_specs = P(None, "lat", "lon")
    return jax.shard_map(local, mesh=mesh, in_specs=in_specs, out_specs=out_specs, check_vma=False)
```

```python
import jax
import jax.numpy as jnp
from jax import lax
from jax.experimental import pallas as pl
from jax.experimental.pallas import tpu as pltpu
from jax.sharding import PartitionSpec as P

SOURCES = 2
LEVELS = 3
MAXS = 4
CH = 3
ROWS = 16
TILES = 8
L = 128

screening = 0.02
damping = 0.8
MESH = pl.DeviceIdType.MESH

T0, T1, T2 = TILES + 1, TILES // 2 + 1, TILES // 4 + 1
O0, R0 = 8, 32
O1, R1 = 24, 56
OP, RP = 8, 32
O2, R2 = 8, 24


def iota(rows, dim):
    return lax.broadcasted_iota(jnp.int32, (rows, L), dim)


def lanes_of(rows):
    lane = iota(rows, 1)
    return lane == 0, lane == L - 1, lane < L // 2


def rolled(x, shift, dim):
    shift %= x.shape[dim]
    return pltpu.roll(x, shift, dim) if shift else x


def residual(src, rhs, c, t, tiles, at, rhs_at, rows, scale):
    diag = screening + 4.0 * scale
    first, last, _ = lanes_of(rows)
    x = src[c, t, at : at + rows]
    before = src[c, (t - 1) % tiles, at : at + rows]
    after = src[c, (t + 1) % tiles, at : at + rows]
    west = rolled(jnp.where(last, before, x), 1, 1)
    east = rolled(jnp.where(first, after, x), -1, 1)
    north = src[c, t, at - 1 : at - 1 + rows]
    south = src[c, t, at + 1 : at + 1 + rows]
    beside = (north + south) + (west + east)
    if scale != 1.0:
        beside = scale * beside
    return x, (rhs[c, t, rhs_at : rhs_at + rows] - diag * x) + beside


def sweep(src, dst, rhs, tiles, at, rhs_at, rows, factor, scale):
    for c in range(CH):
        for t in range(tiles):
            x, r = residual(src, rhs, c, t, tiles, at, rhs_at, rows, scale)
            dst[c, t, at : at + rows] = x + factor * r


def restrict(src, rhs, dst, tmp, tiles, at, rhs_at, rows, dst_at, count, scale):
    low = lanes_of(count)[2]
    pick = (2 * iota(count, 1)) % L
    for c in range(CH):
        for t in range(tiles):
            tmp[c, t, 0:rows] = residual(src, rhs, c, t, tiles, at, rhs_at, rows, scale)[1]
        parts = []
        for t in range(tiles):
            pair = tmp[c, t, pl.ds(0, count, stride=2)] + tmp[c, t, pl.ds(1, count, stride=2)]
            pair = pair + rolled(pair, -1, 1)
            parts.append(0.25 * jnp.take_along_axis(pair, pick, axis=1))
        for t in range(tiles // 2):
            dst[c, t, dst_at : dst_at + count] = jnp.where(low, parts[2 * t], parts[2 * t + 1])
        dst[c, tiles // 2, dst_at : dst_at + count] = parts[-1]


def prolong_rows(src, c, tiles, at, rows, tmp):
    for t in range(tiles):
        x = 0.75 * src[c, t, at : at + rows]
        tmp[c, t, pl.ds(0, rows, stride=2)] = x + 0.25 * src[c, t, at - 1 : at - 1 + rows]
        tmp[c, t, pl.ds(1, rows, stride=2)] = x + 0.25 * src[c, t, at + 1 : at + 1 + rows]


def prolong_cols(xs, rows):
    lane = iota(rows, 1)
    first, last, low = lanes_of(rows)
    aside = jnp.where(lane % 2 == 0, L - 1, 1)
    count = len(xs)
    out = []
    for t in range(count):
        wests = rolled(xs[t - 1], 1, 1)
        easts = rolled(xs[(t + 1) % count], -1, 1)
        for h in range(2 if t < count - 1 else 1):
            here = lane // 2 + (h * (L // 2) if t < count - 1 else jnp.where(low, 0, L // 2))
            near = jnp.take_along_axis(xs[t], here, axis=1)
            far = jnp.take_along_axis(xs[t], (here + aside) % L, axis=1)
            if h == 0:
                far = jnp.where(first, wests, far)
            if h == 1 or t == count - 1:
                far = jnp.where(last, easts, far)
            out.append(0.75 * near + 0.25 * far)
    return out


def kernel(
    sweeps, target, grad_x, grad_y, labels, out,
    gx, gy, lab, v0, w0, b0, sy, sx, ny, ey, wy, wx, xn, xs, xnw, xsw,
    ps, pn, rn, rs, pe, pw, re, rw,
    b1, v1, w1, vp, wp, b2, v2, w2, zn, zs, fn, fs, gn, gs, tmp,
    in_sem, send, recv,
):
    lon, lat = lax.axis_index("lon"), lax.axis_index("lat")
    nlon, nlat = lax.axis_size("lon"), lax.axis_size("lat")

    def peer(dlat, dlon):
        return {"lat": lax.rem(lat + dlat + nlat, nlat), "lon": lax.rem(lon + dlon + nlon, nlon)}

    peers = [(d, 0) for d in (1, -1, 2, -2, 3, -3)]
    peers += [(i, j) for i in (-1, 0, 1) for j in (-1, 1)]
    barrier = pltpu.get_barrier_semaphore()
    for dlat, dlon in peers:
        pl.semaphore_signal(barrier, inc=1, device_id=peer(dlat, dlon), device_id_type=MESH)

    loads = [
        pltpu.make_async_copy(labels, lab, in_sem.at[0]),
        pltpu.make_async_copy(grad_x, gx, in_sem.at[1]),
        pltpu.make_async_copy(grad_y, gy, in_sem.at[2]),
    ]
    for t in range(TILES):
        loads.append(
            pltpu.make_async_copy(
                target.at[:, :, pl.ds(t * L, L)], v0.at[:, t, pl.ds(O0, ROWS)], in_sem.at[3 + t]
            )
        )
    for load in loads:
        load.start()

    used = [0]

    def remote(src, dst, dlat, dlon):
        k = used[0]
        used[0] += 1
        return pltpu.make_async_remote_copy(
            src_ref=src,
            dst_ref=dst,
            send_sem=send.at[k],
            recv_sem=recv.at[k],
            device_id=peer(dlat, dlon),
            device_id_type=MESH,
        )

    first, last, low = lanes_of(ROWS)
    first8, last8, low8 = lanes_of(8)
    sub = iota(8, 0)
    lane = iota(ROWS, 1)
    upper = sub < 4
    row = iota(ROWS, 0)

    def inside(level, start, rows):
        here = iota(rows, 0) + (start + lat * (ROWS >> level))
        return jnp.where((here >= 0) & (here < (nlat * ROWS >> level)), 1.0, 0.0).astype(jnp.float32)

    def step(level, i):
        full = damping / (screening + 4.0 * 0.25**level)
        return jnp.where(sweeps[level] > i, full, 0.0).astype(jnp.float32)

    for c in range(CH):
        for t in range(T0):
            for ref in (v0, w0):
                ref[c, t, 0:8] = jnp.zeros((8, L), jnp.float32)
                ref[c, t, 24:32] = jnp.zeros((8, L), jnp.float32)

    for load in loads[:3]:
        load.wait()

    def picked(ref, c, t, rows):
        cols = slice(t * L, (t + 1) * L)
        return jnp.where(lab[rows, cols] == 0, ref[0, c, rows, cols], ref[1, c, rows, cols])

    for t in range(TILES):
        edge = [rolled(picked(gy, c, t, slice(8, 16)), c + 1, 0) for c in range(CH)]
        sy[t] = jnp.where(sub == 0, edge[0], jnp.where(sub == 1, edge[1], edge[2]))
    edge = [rolled(picked(gx, c, TILES - 1, slice(0, ROWS)), c + 1, 1) for c in range(CH)]
    sx[...] = jnp.where(lane == 0, edge[0], jnp.where(lane == 1, edge[1], edge[2]))

    pl.semaphore_wait(barrier, len(peers))
    north8, south8 = pl.ds(0, 8), pl.ds(8, 8)
    edges = [
        remote(sy, ny.at[pl.ds(0, TILES)], 1, 0),
        remote(sy.at[0], ny.at[TILES], 1, -1),
        remote(sy.at[TILES - 1], ny.at[TILES + 1], 1, 1),
        remote(sy.at[0], ey, 0, -1),
        remote(sy.at[TILES - 1], wy, 0, 1),
        remote(sx, wx, 0, 1),
        remote(sx.at[north8], xs, -1, 0),
        remote(sx.at[south8], xn, 1, 0),
        remote(sx.at[north8], xsw, -1, 1),
        remote(sx.at[south8], xnw, 1, 1),
    ]
    for copy in edges:
        copy.start()
    for load in loads[3:]:
        load.wait()

    own = slice(O0, O0 + ROWS)
    for c in range(CH):
        before = None
        for t in range(TILES):
            x = picked(gx, c, t, slice(0, ROWS))
            y = picked(gy, c, t, slice(0, ROWS))
            moved = rolled(x, 1, 1)
            west = jnp.where(first, 0.0 if t == 0 else before, moved)
            before = moved
            north = jnp.where(row == 0, 0.0, rolled(y, 1, 0))
            v = v0[c, t, own]
            b = screening * v - ((x - west) + (y - north))
            b0[c, t, own] = b
            vn, vs, bn, bs = v[0:8], v[8:16], b[0:8], b[8:16]
            bs = bs + jnp.where(sub == 4, rolled(vs, 1, 0), 0.0)
            ps[c, t] = jnp.where(upper, rolled(bs, 4, 0), vs)
            bn = bn + jnp.where(sub == 3, rolled(vn, -1, 0), 0.0)
            pn[c, t] = jnp.where(upper, vn, rolled(bn, 4, 0))
            if t == 0:
                pw[c] = jnp.where(low, v, rolled(b, L // 2, 1))
            if t == TILES - 1:
                pe[c] = jnp.where(low, rolled(b, L // 2, 1), v)

    e0 = [
        remote(ps, rn.at[:, pl.ds(0, TILES)], 1, 0),
        remote(pn, rs.at[:, pl.ds(0, TILES)], -1, 0),
        remote(pe, rw, 0, 1),
        remote(pw, re, 0, -1),
        remote(ps.at[:, TILES - 1], rn.at[:, TILES + 1], 1, 1),
        remote(ps.at[:, 0], rn.at[:, TILES], 1, -1),
        remote(pn.at[:, TILES - 1], rs.at[:, TILES + 1], -1, 1),
        remote(pn.at[:, 0], rs.at[:, TILES], -1, -1),
    ]
    for copy in e0:
        copy.start()

    inside0 = inside(0, -8, R0)
    has_north = jnp.where(lat > 0, 1.0, 0.0).astype(jnp.float32)
    for copy in edges:
        copy.wait()

    def column(x, c):
        return jnp.where(first if x.shape[0] == ROWS else first8, rolled(x, -c, 1), 0.0)

    def line(x, c):
        return jnp.where(sub == 0, rolled(x, -c, 0), 0.0)

    for c in range(CH):
        b0[c, 0, own] = b0[c, 0, own] + column(wx[...], c)
        for t in range(TILES):
            b0[c, t, 8:16] = b0[c, t, 8:16] + has_north * line(ny[t], c)

    for copy in e0:
        copy.wait()

    for c in range(CH):
        halves = [(rn[c, t], rs[c, t]) for t in range(TILES)]
        halves.append(
            (jnp.where(low8, rn[c, TILES], rn[c, TILES + 1]), jnp.where(low8, rs[c, TILES], rs[c, TILES + 1]))
        )
        for t, (n, s) in enumerate(halves):
            v0[c, t, 0:8] = jnp.where(upper, 0.0, n) * inside0[0:8]
            v0[c, t, 24:32] = jnp.where(upper, s, 0.0) * inside0[24:32]
            n, s = rolled(n, 4, 0), rolled(s, 4, 0)
            below = sy[t] if t < TILES else jnp.where(low8, ey[...], wy[...])
            s = s + line(below, c)
            if t == 0:
                n, s = n + column(xnw[...], c), s + column(xsw[...], c)
            if t == TILES:
                n, s = n + column(xn[...], c), s + column(xs[...], c)
            b0[c, t, 0:8] = n
            b0[c, t, 24:32] = s
        v0[c, TILES, own] = jnp.where(low, re[c], rw[c])
        b = rolled(jnp.where(low, rw[c], re[c]), L // 2, 1) + column(sx[...], c)
        above = has_north * line(jnp.where(low8, ny[TILES], ny[TILES + 1]), c)
        b0[c, TILES, 8:16] = b[0:8] + above
        b0[c, TILES, 16:24] = b[8:16]

    for i in range(MAXS):
        a, b = (v0, w0) if i % 2 == 0 else (w0, v0)
        sweep(a, b, b0, T0, 4, 4, 24, inside0[4:28] * step(0, i), 1.0)

    restrict(v0, b0, b1, tmp, T0, O0, O0, ROWS, O1, 8, 1.0)
    for t in range(T1):
        rows = [b1[c, t, O1 : O1 + 8] for c in range(CH)]
        n, s = ([rolled(x, 2 * c + k, 0) for c, x in enumerate(rows)] for k in (0, 2))
        fn[t] = jnp.where(sub < 2, n[0], jnp.where(upper, n[1], n[2]))
        fs[t] = jnp.where(sub < 2, s[0], jnp.where(upper, s[1], s[2]))
    mine = b1.at[:, :, pl.ds(O1, 8)]
    e1 = [remote(mine, b1.at[:, :, pl.ds(O1 - 8 * d, 8)], d, 0) for d in (2, -2)]
    e1 += [remote(fs, gn, 3, 0), remote(fn, gs, -3, 0)]
    e1 += [remote(mine, b1.at[:, :, pl.ds(O1 - 8 * d, 8)], d, 0) for d in (1, -1)]
    e2 = [
        remote(v0.at[:, :, pl.ds(O0, 8)], zs, -1, 0),
        remote(v0.at[:, :, pl.ds(O0 + 8, 8)], zn, 1, 0),
    ]
    for copy in e1 + e2:
        copy.start()

    def factor(level, i, base, at, rows):
        return inside(level, at - base, rows) * step(level, i)

    for copy in e1:
        copy.wait()
    for c in range(CH):
        for t in range(T1):
            b1[c, t, 0:8] = rolled(gn[t], -2 * c - 2, 0)
            b1[c, t, 48:56] = rolled(gs[t], -2 * c, 0)

    f = factor(1, 0, O1, 0, R1)
    for c in range(CH):
        for t in range(T1):
            v1[c, t] = f * b1[c, t]
    sweep(v1, w1, b1, T1, 4, 4, 48, factor(1, 1, O1, 4, 48), 0.25)
    sweep(w1, v1, b1, T1, 8, 8, 40, factor(1, 2, O1, 8, 40), 0.25)
    sweep(v1, w1, b1, T1, 8, 8, 40, factor(1, 3, O1, 8, 40), 0.25)
    for c in range(CH):
        for t in range(T1):
            tmp[c, t, 40:48] = jnp.zeros((8, L), jnp.float32)
    restrict(w1, b1, b2, tmp, T1, 8, 8, 40, 0, R2, 0.25)

    f = factor(2, 0, O2, 0, R2)
    for c in range(CH):
        for t in range(T2):
            v2[c, t] = f * b2[c, t]
    for i in range(1, MAXS):
        a, b = (v2, w2) if i % 2 else (w2, v2)
        sweep(a, b, b2, T2, 2, 2, 16, factor(2, i, O2, 2, 16), 0.0625)

    insidep = inside(1, -OP, 24)
    for c in range(CH):
        prolong_rows(w2, c, T2, 4, 16, tmp)
        fine = prolong_cols([tmp[c, t, 0:24] for t in range(T2)], 24)
        for t in range(T1):
            vp[c, t, 0:24] = (w1[c, t, 16:40] + fine[t]) * insidep
    for i, (at, rows) in enumerate(((1, 24), (1, 24), (4, 16), (4, 16))):
        a, b = (vp, wp) if i % 2 == 0 else (wp, vp)
        sweep(a, b, b1, T1, at, at + O1 - OP, rows, factor(1, i, OP, at, rows), 0.25)

    for copy in e2:
        copy.wait()
    for c in range(CH):
        prolong_rows(vp, c, T1, 4, 16, tmp)
        fine = prolong_cols([tmp[c, t, 0:32] for t in range(T1)], 32)
        for t in range(T0):
            v0[c, t, 0:8] = (zn[c, t] + fine[t][0:8]) * inside0[0:8]
            v0[c, t, own] = v0[c, t, own] + fine[t][8:24]
            v0[c, t, 24:32] = (zs[c, t] + fine[t][24:32]) * inside0[24:32]
    for i in range(MAXS - 1):
        a, b = (v0, w0) if i % 2 == 0 else (w0, v0)
        sweep(a, b, b0, T0, 4, 4, 24, inside0[4:28] * step(0, i), 1.0)
    f = step(0, MAXS - 1)
    for c in range(CH):
        for t in range(TILES):
            x, r = residual(w0, b0, c, t, T0, O0, O0, ROWS, 1.0)
            out[c, :, t * L : (t + 1) * L] = x + f * r


def local(target, grad_x, grad_y, labels, sweeps):
    f32 = jnp.float32

    def vmem(*shape):
        return pltpu.VMEM(shape + (L,), f32)

    scratch = [
        pltpu.VMEM(grad_x.shape, f32),
        pltpu.VMEM(grad_y.shape, f32),
        pltpu.VMEM(labels.shape, jnp.int32),
        vmem(CH, T0, R0), vmem(CH, T0, R0), vmem(CH, T0, R0),
        vmem(TILES, 8), vmem(ROWS),
        vmem(TILES + 2, 8), vmem(8), vmem(8), vmem(ROWS),
        vmem(8), vmem(8), vmem(8), vmem(8),
        vmem(CH, TILES, 8), vmem(CH, TILES, 8),
        vmem(CH, TILES + 2, 8), vmem(CH, TILES + 2, 8),
        vmem(CH, ROWS), vmem(CH, ROWS), vmem(CH, ROWS), vmem(CH, ROWS),
        vmem(CH, T1, R1), vmem(CH, T1, R1), vmem(CH, T1, R1),
        vmem(CH, T1, RP), vmem(CH, T1, RP),
        vmem(CH, T2, R2), vmem(CH, T2, R2), vmem(CH, T2, R2),
        vmem(CH, T0, 8), vmem(CH, T0, 8),
        vmem(T1, 8), vmem(T1, 8), vmem(T1, 8), vmem(T1, 8),
        vmem(CH, T0, 48),
        pltpu.SemaphoreType.DMA((3 + TILES,)),
        pltpu.SemaphoreType.DMA((26,)),
        pltpu.SemaphoreType.DMA((26,)),
    ]
    anywhere = pl.BlockSpec(memory_space=pl.ANY)
    return pl.pallas_call(
        kernel,
        out_shape=jax.ShapeDtypeStruct(target.shape, f32),
        in_specs=[pl.BlockSpec(memory_space=pltpu.SMEM)] + [anywhere] * 4,
        out_specs=pl.BlockSpec(memory_space=pltpu.VMEM),
        scratch_shapes=scratch,
        compiler_params=pltpu.CompilerParams(collective_id=0, has_side_effects=True),
        name="vcycle",
    )(sweeps, target, grad_x, grad_y, labels)


def solution(mesh):
    in_specs = (
        P(None, "lat", "lon"),
        P(None, None, "lat", "lon"),
        P(None, None, "lat", "lon"),
        P("lat", "lon"),
        P(),
    )
    out_specs = P(None, "lat", "lon")
    return jax.shard_map(local, mesh=mesh, in_specs=in_specs, out_specs=out_specs, check_vma=False)
```

```python
import jax
import jax.numpy as jnp
from jax import lax
from jax.experimental import pallas as pl
from jax.experimental.pallas import tpu as pltpu
from jax.sharding import PartitionSpec as P

SOURCES = 2
LEVELS = 3
MAXS = 4
CH = 3
ROWS = 16
TILES = 8
L = 128

screening = 0.02
damping = 0.8
MESH = pl.DeviceIdType.MESH

T0, T1, T2 = TILES + 1, TILES // 2 + 1, TILES // 4 + 1
O0, R0 = 8, 32
O1, R1 = 24, 56
OP, RP = 8, 32
O2, R2 = 8, 24
WIDE = 21


def iota(rows, dim):
    return lax.broadcasted_iota(jnp.int32, (rows, L), dim)


def lanes_of(rows):
    lane = iota(rows, 1)
    return lane == 0, lane == L - 1, lane < L // 2


def rolled(x, shift, dim):
    shift %= x.shape[dim]
    return pltpu.roll(x, shift, dim) if shift else x


def residual(src, rhs, c, t, tiles, at, rhs_at, rows, scale):
    diag = screening + 4.0 * scale
    first, last, _ = lanes_of(rows)
    x = src[c, t, at : at + rows]
    before = src[c, (t - 1) % tiles, at : at + rows]
    after = src[c, (t + 1) % tiles, at : at + rows]
    west = rolled(jnp.where(last, before, x), 1, 1)
    east = rolled(jnp.where(first, after, x), -1, 1)
    north = src[c, t, at - 1 : at - 1 + rows]
    south = src[c, t, at + 1 : at + 1 + rows]
    beside = (north + south) + (west + east)
    if scale != 1.0:
        beside = scale * beside
    return x, (rhs[c, t, rhs_at : rhs_at + rows] - diag * x) + beside


def sweep(src, dst, rhs, tiles, at, rhs_at, rows, factor, scale):
    for c in range(CH):
        for t in range(tiles):
            x, r = residual(src, rhs, c, t, tiles, at, rhs_at, rows, scale)
            dst[c, t, at : at + rows] = x + factor * r


def restrict(src, rhs, dst, tmp, tiles, at, rhs_at, rows, dst_at, count, scale):
    low = lanes_of(count)[2]
    pick = (2 * iota(count, 1)) % L
    for c in range(CH):
        for t in range(tiles):
            tmp[c, t, 0:rows] = residual(src, rhs, c, t, tiles, at, rhs_at, rows, scale)[1]
        parts = []
        for t in range(tiles):
            pair = tmp[c, t, pl.ds(0, count, stride=2)] + tmp[c, t, pl.ds(1, count, stride=2)]
            pair = pair + rolled(pair, -1, 1)
            parts.append(0.25 * jnp.take_along_axis(pair, pick, axis=1))
        for t in range(tiles // 2):
            dst[c, t, dst_at : dst_at + count] = jnp.where(low, parts[2 * t], parts[2 * t + 1])
        dst[c, tiles // 2, dst_at : dst_at + count] = parts[-1]


def prolong_rows(src, c, tiles, at, rows, tmp):
    for t in range(tiles):
        x = 0.75 * src[c, t, at : at + rows]
        tmp[c, t, pl.ds(0, rows, stride=2)] = x + 0.25 * src[c, t, at - 1 : at - 1 + rows]
        tmp[c, t, pl.ds(1, rows, stride=2)] = x + 0.25 * src[c, t, at + 1 : at + 1 + rows]


def prolong_cols(xs, rows):
    lane = iota(rows, 1)
    first, last, low = lanes_of(rows)
    aside = jnp.where(lane % 2 == 0, L - 1, 1)
    count = len(xs)
    out = []
    for t in range(count):
        wests = rolled(xs[t - 1], 1, 1)
        easts = rolled(xs[(t + 1) % count], -1, 1)
        for h in range(2 if t < count - 1 else 1):
            here = lane // 2 + (h * (L // 2) if t < count - 1 else jnp.where(low, 0, L // 2))
            near = jnp.take_along_axis(xs[t], here, axis=1)
            far = jnp.take_along_axis(xs[t], (here + aside) % L, axis=1)
            if h == 0:
                far = jnp.where(first, wests, far)
            if h == 1 or t == count - 1:
                far = jnp.where(last, easts, far)
            out.append(0.75 * near + 0.25 * far)
    return out


def kernel(
    sweeps, target, grad_x, grad_y, labels, out,
    gx, gy, lab, v0, w0, b0, sy, sx, ny, ey, wy, wx, xn, xs, xnw, xsw,
    ps, pn, rn, rs, pe, pw, re, rw,
    b1, v1, w1, vp, wp, b2, v2, w2, zn, zs, un, us, hs, fn, fs, gn, gs, tmp,
    in_sem, send, recv,
):
    lon, lat = lax.axis_index("lon"), lax.axis_index("lat")
    nlon, nlat = lax.axis_size("lon"), lax.axis_size("lat")

    def peer(dlat, dlon):
        return {"lat": lax.rem(lat + dlat + nlat, nlat), "lon": lax.rem(lon + dlon + nlon, nlon)}

    peers = [(d, 0) for d in (1, -1, 2, -2, 3, -3)]
    peers += [(i, j) for i in (-1, 0, 1) for j in (-1, 1)]
    barrier = pltpu.get_barrier_semaphore()
    for dlat, dlon in peers:
        pl.semaphore_signal(barrier, inc=1, device_id=peer(dlat, dlon), device_id_type=MESH)

    loads = [
        pltpu.make_async_copy(labels, lab, in_sem.at[0]),
        pltpu.make_async_copy(grad_x, gx, in_sem.at[1]),
        pltpu.make_async_copy(grad_y, gy, in_sem.at[2]),
    ]
    for t in range(TILES):
        loads.append(
            pltpu.make_async_copy(
                target.at[:, :, pl.ds(t * L, L)], v0.at[:, t, pl.ds(O0, ROWS)], in_sem.at[3 + t]
            )
        )
    for load in loads:
        load.start()

    used = [0]

    def remote(src, dst, dlat, dlon):
        k = used[0]
        used[0] += 1
        return pltpu.make_async_remote_copy(
            src_ref=src,
            dst_ref=dst,
            send_sem=send.at[k],
            recv_sem=recv.at[k],
            device_id=peer(dlat, dlon),
            device_id_type=MESH,
        )

    first, last, low = lanes_of(ROWS)
    first8, last8, low8 = lanes_of(8)
    low4 = lanes_of(4)[2]
    sub = iota(8, 0)
    lane, lane8 = iota(ROWS, 1), iota(8, 1)
    upper = sub < 4
    row = iota(ROWS, 0)

    def inside(level, start, rows):
        here = iota(rows, 0) + (start + lat * (ROWS >> level))
        return jnp.where((here >= 0) & (here < (nlat * ROWS >> level)), 1.0, 0.0).astype(jnp.float32)

    def step(level, i):
        full = damping / (screening + 4.0 * 0.25**level)
        return jnp.where(sweeps[level] > i, full, 0.0).astype(jnp.float32)

    for c in range(CH):
        for t in range(T0):
            for ref in (v0, w0):
                ref[c, t, 0:8] = jnp.zeros((8, L), jnp.float32)
                ref[c, t, 24:32] = jnp.zeros((8, L), jnp.float32)

    for load in loads[:3]:
        load.wait()

    def picked(ref, c, t, rows):
        cols = slice(t * L, (t + 1) * L)
        return jnp.where(lab[rows, cols] == 0, ref[0, c, rows, cols], ref[1, c, rows, cols])

    for t in range(TILES):
        edge = [rolled(picked(gy, c, t, slice(8, 16)), c + 1, 0) for c in range(CH)]
        sy[t] = jnp.where(sub == 0, edge[0], jnp.where(sub == 1, edge[1], edge[2]))[0:4]
    edge = [rolled(picked(gx, c, TILES - 1, slice(0, ROWS)), c + 1, 1) for c in range(CH)]
    sx[...] = jnp.where(lane == 0, edge[0], jnp.where(lane == 1, edge[1], edge[2]))

    pl.semaphore_wait(barrier, len(peers))
    north8, south8 = pl.ds(0, 8), pl.ds(8, 8)
    edges = [
        remote(sy, ny.at[pl.ds(0, TILES)], 1, 0),
        remote(sy.at[0], ny.at[TILES], 1, -1),
        remote(sy.at[TILES - 1], ny.at[TILES + 1], 1, 1),
        remote(sy.at[0], ey, 0, -1),
        remote(sy.at[TILES - 1], wy, 0, 1),
        remote(sx, wx, 0, 1),
        remote(sx.at[north8], xs, -1, 0),
        remote(sx.at[south8], xn, 1, 0),
        remote(sx.at[north8], xsw, -1, 1),
        remote(sx.at[south8], xnw, 1, 1),
    ]
    for copy in edges:
        copy.start()
    for load in loads[3:]:
        load.wait()

    own = slice(O0, O0 + ROWS)
    for c in range(CH):
        before = None
        for t in range(TILES):
            x = picked(gx, c, t, slice(0, ROWS))
            y = picked(gy, c, t, slice(0, ROWS))
            moved = rolled(x, 1, 1)
            west = jnp.where(first, 0.0 if t == 0 else before, moved)
            before = moved
            north = jnp.where(row == 0, 0.0, rolled(y, 1, 0))
            v = v0[c, t, own]
            b = screening * v - ((x - west) + (y - north))
            b0[c, t, own] = b
            vn, vs, bn, bs = v[0:8], v[8:16], b[0:8], b[8:16]
            bs = bs + jnp.where(sub == 4, rolled(vs, 1, 0), 0.0)
            ps[c, t] = jnp.where(upper, rolled(bs, 4, 0), vs)
            bn = bn + jnp.where(sub == 3, rolled(vn, -1, 0), 0.0)
            pn[c, t] = jnp.where(upper, vn, rolled(bn, 4, 0))
            if t == 0:
                pw[c] = jnp.where(low, v, rolled(b, L // 2, 1))
            if t == TILES - 1:
                pe[c] = jnp.where(low, rolled(b, L // 2, 1), v)

    e0 = [
        remote(ps, rn.at[:, pl.ds(0, TILES)], 1, 0),
        remote(pn, rs.at[:, pl.ds(0, TILES)], -1, 0),
        remote(pe, rw, 0, 1),
        remote(pw, re, 0, -1),
        remote(ps.at[:, TILES - 1], rn.at[:, TILES + 1], 1, 1),
        remote(ps.at[:, 0], rn.at[:, TILES], 1, -1),
        remote(pn.at[:, TILES - 1], rs.at[:, TILES + 1], -1, 1),
        remote(pn.at[:, 0], rs.at[:, TILES], -1, -1),
    ]
    for copy in e0:
        copy.start()

    inside0 = inside(0, -8, R0)
    has_north = jnp.where(lat > 0, 1.0, 0.0).astype(jnp.float32)
    for copy in edges:
        copy.wait()

    def column(x, c):
        return jnp.where(first if x.shape[0] == ROWS else first8, rolled(x, -c, 1), 0.0)

    def line(x, c):
        return jnp.where(sub == 0, x[c : c + 1], 0.0)

    for c in range(CH):
        b0[c, 0, own] = b0[c, 0, own] + column(wx[...], c)
        for t in range(TILES):
            b0[c, t, 8:16] = b0[c, t, 8:16] + has_north * line(ny[t], c)

    for copy in e0:
        copy.wait()

    for c in range(CH):
        halves = [(rn[c, t], rs[c, t]) for t in range(TILES)]
        halves.append(
            (jnp.where(low8, rn[c, TILES], rn[c, TILES + 1]), jnp.where(low8, rs[c, TILES], rs[c, TILES + 1]))
        )
        for t, (n, s) in enumerate(halves):
            v0[c, t, 0:8] = jnp.where(upper, 0.0, n) * inside0[0:8]
            v0[c, t, 24:32] = jnp.where(upper, s, 0.0) * inside0[24:32]
            n, s = rolled(n, 4, 0), rolled(s, 4, 0)
            below = sy[t] if t < TILES else jnp.where(low4, ey[...], wy[...])
            s = s + line(below, c)
            if t == 0:
                n, s = n + column(xnw[...], c), s + column(xsw[...], c)
            if t == TILES:
                n, s = n + column(xn[...], c), s + column(xs[...], c)
            b0[c, t, 0:8] = n
            b0[c, t, 24:32] = s
        v0[c, TILES, own] = jnp.where(low, re[c], rw[c])
        b = rolled(jnp.where(low, rw[c], re[c]), L // 2, 1) + column(sx[...], c)
        above = has_north * line(jnp.where(low4, ny[TILES], ny[TILES + 1]), c)
        b0[c, TILES, 8:16] = b[0:8] + above
        b0[c, TILES, 16:24] = b[8:16]

    for i in range(MAXS):
        a, b = (v0, w0) if i % 2 == 0 else (w0, v0)
        sweep(a, b, b0, T0, 4, 4, 24, inside0[4:28] * step(0, i), 1.0)

    restrict(v0, b0, b1, tmp, T0, O0, O0, ROWS, O1, 8, 1.0)
    for t in range(T1):
        rows = [b1[c, t, O1 : O1 + 8] for c in range(CH)]
        n, s = ([rolled(x, 2 * c + k, 0) for c, x in enumerate(rows)] for k in (0, 2))
        fn[t] = jnp.where(sub < 2, n[0], jnp.where(upper, n[1], n[2]))
        fs[t] = jnp.where(sub < 2, s[0], jnp.where(upper, s[1], s[2]))
    turned = [rolled(b1[c, T1 - 1, O1 : O1 + 8], WIDE + 2 * WIDE * c, 1) for c in range(CH)]
    hs[O1 : O1 + 8] = jnp.where(lane8 < 2 * WIDE, turned[0], jnp.where(lane8 < 4 * WIDE, turned[1], turned[2]))

    def sent(d):
        rows, there = pl.ds(O1, 8), pl.ds(O1 - 8 * d, 8)
        return [
            remote(b1.at[:, pl.ds(0, T1 - 1), rows], b1.at[:, pl.ds(0, T1 - 1), there], d, 0),
            remote(hs.at[rows], hs.at[there], d, 0),
        ]

    e1 = sent(2) + sent(-2)
    e1 += [remote(fs, gn, 3, 0), remote(fn, gs, -3, 0)]
    e1 += sent(1) + sent(-1)
    e2 = [
        remote(un, zs, -1, 0),
        remote(us, zn, 1, 0),
    ]
    for copy in e1:
        copy.start()
    for c in range(CH):
        for t in range(T0):
            un[c, t] = v0[c, t, O0 : O0 + 4]
            us[c, t] = v0[c, t, O0 + ROWS - 4 : O0 + ROWS]
    for copy in e2:
        copy.start()

    def factor(level, i, base, at, rows):
        return inside(level, at - base, rows) * step(level, i)

    for copy in e1:
        copy.wait()
    for c in range(CH):
        for t in range(T1):
            b1[c, t, 0:8] = rolled(gn[t], -2 * c - 2, 0)
            b1[c, t, 48:56] = rolled(gs[t], -2 * c, 0)
        for at, rows in ((8, 16), (32, 16)):
            b1[c, T1 - 1, at : at + rows] = rolled(hs[at : at + rows], -WIDE - 2 * WIDE * c, 1)

    f = factor(1, 0, O1, 0, R1)
    for c in range(CH):
        for t in range(T1):
            v1[c, t] = f * b1[c, t]
    sweep(v1, w1, b1, T1, 4, 4, 48, factor(1, 1, O1, 4, 48), 0.25)
    sweep(w1, v1, b1, T1, 8, 8, 40, factor(1, 2, O1, 8, 40), 0.25)
    sweep(v1, w1, b1, T1, 8, 8, 40, factor(1, 3, O1, 8, 40), 0.25)
    for c in range(CH):
        for t in range(T1):
            tmp[c, t, 40:48] = jnp.zeros((8, L), jnp.float32)
    restrict(w1, b1, b2, tmp, T1, 8, 8, 40, 0, R2, 0.25)

    f = factor(2, 0, O2, 0, R2)
    for c in range(CH):
        for t in range(T2):
            v2[c, t] = f * b2[c, t]
    for i in range(1, MAXS):
        a, b = (v2, w2) if i % 2 else (w2, v2)
        sweep(a, b, b2, T2, 2, 2, 16, factor(2, i, O2, 2, 16), 0.0625)

    insidep = inside(1, -OP, 24)
    for c in range(CH):
        prolong_rows(w2, c, T2, 4, 16, tmp)
        fine = prolong_cols([tmp[c, t, 0:24] for t in range(T2)], 24)
        for t in range(T1):
            vp[c, t, 0:24] = (w1[c, t, 16:40] + fine[t]) * insidep
    for i, (at, rows) in enumerate(((1, 24), (1, 24), (4, 16), (4, 16))):
        a, b = (vp, wp) if i % 2 == 0 else (wp, vp)
        sweep(a, b, b1, T1, at, at + O1 - OP, rows, factor(1, i, OP, at, rows), 0.25)

    for copy in e2:
        copy.wait()
    for c in range(CH):
        prolong_rows(vp, c, T1, 4, 16, tmp)
        fine = prolong_cols([tmp[c, t, 0:32] for t in range(T1)], 32)
        for t in range(T0):
            v0[c, t, 4:8] = (zn[c, t] + fine[t][4:8]) * inside0[4:8]
            v0[c, t, own] = v0[c, t, own] + fine[t][8:24]
            v0[c, t, 24:28] = (zs[c, t] + fine[t][24:28]) * inside0[24:28]
    for i in range(MAXS - 1):
        a, b = (v0, w0) if i % 2 == 0 else (w0, v0)
        sweep(a, b, b0, T0, 4, 4, 24, inside0[4:28] * step(0, i), 1.0)
    f = step(0, MAXS - 1)
    for c in range(CH):
        for t in range(TILES):
            x, r = residual(w0, b0, c, t, T0, O0, O0, ROWS, 1.0)
            out[c, :, t * L : (t + 1) * L] = x + f * r


def local(target, grad_x, grad_y, labels, sweeps):
    f32 = jnp.float32

    def vmem(*shape):
        return pltpu.VMEM(shape + (L,), f32)

    scratch = [
        pltpu.VMEM(grad_x.shape, f32),
        pltpu.VMEM(grad_y.shape, f32),
        pltpu.VMEM(labels.shape, jnp.int32),
        vmem(CH, T0, R0), vmem(CH, T0, R0), vmem(CH, T0, R0),
        vmem(TILES, 4), vmem(ROWS),
        vmem(TILES + 2, 4), vmem(4), vmem(4), vmem(ROWS),
        vmem(8), vmem(8), vmem(8), vmem(8),
        vmem(CH, TILES, 8), vmem(CH, TILES, 8),
        vmem(CH, TILES + 2, 8), vmem(CH, TILES + 2, 8),
        vmem(CH, ROWS), vmem(CH, ROWS), vmem(CH, ROWS), vmem(CH, ROWS),
        vmem(CH, T1, R1), vmem(CH, T1, R1), vmem(CH, T1, R1),
        vmem(CH, T1, RP), vmem(CH, T1, RP),
        vmem(CH, T2, R2), vmem(CH, T2, R2), vmem(CH, T2, R2),
        vmem(CH, T0, 4), vmem(CH, T0, 4), vmem(CH, T0, 4), vmem(CH, T0, 4),
        vmem(R1),
        vmem(T1, 8), vmem(T1, 8), vmem(T1, 8), vmem(T1, 8),
        vmem(CH, T0, 48),
        pltpu.SemaphoreType.DMA((3 + TILES,)),
        pltpu.SemaphoreType.DMA((32,)),
        pltpu.SemaphoreType.DMA((32,)),
    ]
    anywhere = pl.BlockSpec(memory_space=pl.ANY)
    return pl.pallas_call(
        kernel,
        out_shape=jax.ShapeDtypeStruct(target.shape, f32),
        in_specs=[pl.BlockSpec(memory_space=pltpu.SMEM)] + [anywhere] * 4,
        out_specs=pl.BlockSpec(memory_space=pltpu.VMEM),
        scratch_shapes=scratch,
        compiler_params=pltpu.CompilerParams(collective_id=0, has_side_effects=True),
        name="vcycle",
    )(sweeps, target, grad_x, grad_y, labels)


def solution(mesh):
    in_specs = (
        P(None, "lat", "lon"),
        P(None, None, "lat", "lon"),
        P(None, None, "lat", "lon"),
        P("lat", "lon"),
        P(),
    )
    out_specs = P(None, "lat", "lon")
    return jax.shard_map(local, mesh=mesh, in_specs=in_specs, out_specs=out_specs, check_vma=False)
```

```python
import jax
import jax.numpy as jnp
from jax import lax
from jax.experimental import pallas as pl
from jax.experimental.pallas import tpu as pltpu
from jax.sharding import PartitionSpec as P

SOURCES = 2
LEVELS = 3
MAXS = 4
CH = 3
ROWS = 16
TILES = 8
L = 128

screening = 0.02
damping = 0.8
MESH = pl.DeviceIdType.MESH

T0, T1, T2 = TILES + 1, TILES // 2 + 1, TILES // 4 + 1
O0, R0 = 8, 32
O1, R1 = 24, 56
OP, RP = 8, 32
O2, R2 = 8, 24
WIDE = 21


def iota(rows, dim):
    return lax.broadcasted_iota(jnp.int32, (rows, L), dim)


def lanes_of(rows):
    lane = iota(rows, 1)
    return lane == 0, lane == L - 1, lane < L // 2


def rolled(x, shift, dim):
    shift %= x.shape[dim]
    return pltpu.roll(x, shift, dim) if shift else x


def residual(src, rhs, c, t, tiles, at, rhs_at, rows, scale):
    diag = screening + 4.0 * scale
    first, last, _ = lanes_of(rows)
    x = src[c, t, at : at + rows]
    before = src[c, (t - 1) % tiles, at : at + rows]
    after = src[c, (t + 1) % tiles, at : at + rows]
    west = rolled(jnp.where(last, before, x), 1, 1)
    east = rolled(jnp.where(first, after, x), -1, 1)
    north = src[c, t, at - 1 : at - 1 + rows]
    south = src[c, t, at + 1 : at + 1 + rows]
    beside = (north + south) + (west + east)
    if scale != 1.0:
        beside = scale * beside
    return x, (rhs[c, t, rhs_at : rhs_at + rows] - diag * x) + beside


def sweep(src, dst, rhs, tiles, at, rhs_at, rows, factor, scale):
    for c in range(CH):
        for t in range(tiles):
            x, r = residual(src, rhs, c, t, tiles, at, rhs_at, rows, scale)
            dst[c, t, at : at + rows] = x + factor * r


def restrict(src, rhs, dst, tmp, tiles, at, rhs_at, rows, dst_at, count, scale):
    low = lanes_of(count)[2]
    pick = (2 * iota(count, 1)) % L
    for c in range(CH):
        for t in range(tiles):
            tmp[c, t, 0:rows] = residual(src, rhs, c, t, tiles, at, rhs_at, rows, scale)[1]
        parts = []
        for t in range(tiles):
            pair = tmp[c, t, pl.ds(0, count, stride=2)] + tmp[c, t, pl.ds(1, count, stride=2)]
            pair = pair + rolled(pair, -1, 1)
            parts.append(0.25 * jnp.take_along_axis(pair, pick, axis=1))
        for t in range(tiles // 2):
            dst[c, t, dst_at : dst_at + count] = jnp.where(low, parts[2 * t], parts[2 * t + 1])
        dst[c, tiles // 2, dst_at : dst_at + count] = parts[-1]


def prolong_rows(src, c, tiles, at, rows, tmp):
    for t in range(tiles):
        x = 0.75 * src[c, t, at : at + rows]
        tmp[c, t, pl.ds(0, rows, stride=2)] = x + 0.25 * src[c, t, at - 1 : at - 1 + rows]
        tmp[c, t, pl.ds(1, rows, stride=2)] = x + 0.25 * src[c, t, at + 1 : at + 1 + rows]


def prolong_cols(xs, rows):
    lane = iota(rows, 1)
    first, last, low = lanes_of(rows)
    aside = jnp.where(lane % 2 == 0, L - 1, 1)
    count = len(xs)
    out = []
    for t in range(count):
        wests = rolled(xs[t - 1], 1, 1)
        easts = rolled(xs[(t + 1) % count], -1, 1)
        for h in range(2 if t < count - 1 else 1):
            here = lane // 2 + (h * (L // 2) if t < count - 1 else jnp.where(low, 0, L // 2))
            near = jnp.take_along_axis(xs[t], here, axis=1)
            far = jnp.take_along_axis(xs[t], (here + aside) % L, axis=1)
            if h == 0:
                far = jnp.where(first, wests, far)
            if h == 1 or t == count - 1:
                far = jnp.where(last, easts, far)
            out.append(0.75 * near + 0.25 * far)
    return out


def kernel(
    counts, target, grad_x, grad_y, labels, out,
    gx, gy, lab, v0, w0, b0, sy, sx, ny, ey, wy, wx, xn, xs, xnw, xsw,
    ps, pn, rn, rs, pe, pw, re, rw,
    b1, v1, w1, vp, wp, b2, v2, w2, zn, zs, un, us, hs, fn, fs, gn, gs, tmp,
    sweeps, in_sem, send, recv,
):
    lon, lat = lax.axis_index("lon"), lax.axis_index("lat")
    nlon, nlat = lax.axis_size("lon"), lax.axis_size("lat")

    def peer(dlat, dlon):
        return {"lat": lax.rem(lat + dlat + nlat, nlat), "lon": lax.rem(lon + dlon + nlon, nlon)}

    peers = [(d, 0) for d in (1, -1, 2, -2, 3, -3)]
    peers += [(i, j) for i in (-1, 0, 1) for j in (-1, 1)]
    barrier = pltpu.get_barrier_semaphore()
    for dlat, dlon in peers:
        pl.semaphore_signal(barrier, inc=1, device_id=peer(dlat, dlon), device_id_type=MESH)

    loads = []

    def load(src, dst):
        loads.append(pltpu.make_async_copy(src, dst, in_sem.at[len(loads)]))

    for tiles, cols in (((0,), pl.ds(0, L)), ((TILES - 1,), pl.ds((TILES - 2) * L, 2 * L))):
        load(grad_x.at[:, :, :, cols], gx.at[:, :, :, cols])
        load(grad_y.at[:, :, :, cols], gy.at[:, :, :, cols])
        load(labels.at[:, cols], lab.at[:, cols])
        for t in tiles:
            load(target.at[:, :, pl.ds(t * L, L)], v0.at[:, t, pl.ds(O0, ROWS)])
    edge_loads = len(loads)
    cols = pl.ds(L, (TILES - 3) * L)
    load(grad_x.at[:, :, :, cols], gx.at[:, :, :, cols])
    load(grad_y.at[:, :, :, cols], gy.at[:, :, :, cols])
    load(labels.at[:, cols], lab.at[:, cols])
    for t in range(1, TILES - 1):
        load(target.at[:, :, pl.ds(t * L, L)], v0.at[:, t, pl.ds(O0, ROWS)])
    load(counts, sweeps)
    for copy in loads:
        copy.start()

    used = [0]

    def remote(src, dst, dlat, dlon):
        k = used[0]
        used[0] += 1
        return pltpu.make_async_remote_copy(
            src_ref=src,
            dst_ref=dst,
            send_sem=send.at[k],
            recv_sem=recv.at[k],
            device_id=peer(dlat, dlon),
            device_id_type=MESH,
        )

    first, last, low = lanes_of(ROWS)
    first8, last8, low8 = lanes_of(8)
    low4 = lanes_of(4)[2]
    sub = iota(8, 0)
    lane, lane8 = iota(ROWS, 1), iota(8, 1)
    upper = sub < 4
    row = iota(ROWS, 0)

    def inside(level, start, rows):
        here = iota(rows, 0) + (start + lat * (ROWS >> level))
        return jnp.where((here >= 0) & (here < (nlat * ROWS >> level)), 1.0, 0.0).astype(jnp.float32)

    def step(level, i):
        full = damping / (screening + 4.0 * 0.25**level)
        return jnp.where(sweeps[level] > i, full, 0.0).astype(jnp.float32)

    for c in range(CH):
        for t in range(T0):
            for ref in (v0, w0):
                ref[c, t, 0:8] = jnp.zeros((8, L), jnp.float32)
                ref[c, t, 24:32] = jnp.zeros((8, L), jnp.float32)

    for copy in loads[:edge_loads]:
        copy.wait()

    def picked(ref, c, t, rows):
        cols = slice(t * L, (t + 1) * L)
        return jnp.where(lab[rows, cols] == 0, ref[0, c, rows, cols], ref[1, c, rows, cols])

    def south_edge(t):
        edge = [rolled(picked(gy, c, t, slice(8, 16)), c + 1, 0) for c in range(CH)]
        sy[t] = jnp.where(sub == 0, edge[0], jnp.where(sub == 1, edge[1], edge[2]))[0:4]

    own = slice(O0, O0 + ROWS)
    all_rows = slice(0, ROWS)

    def right_side(c, t):
        x = picked(gx, c, t, all_rows)
        y = picked(gy, c, t, all_rows)
        before = 0.0 if t == 0 else rolled(picked(gx, c, t - 1, all_rows), 1, 1)
        west = jnp.where(first, before, rolled(x, 1, 1))
        north = jnp.where(row == 0, 0.0, rolled(y, 1, 0))
        v = v0[c, t, own]
        b = screening * v - ((x - west) + (y - north))
        b0[c, t, own] = b
        vn, vs, bn, bs = v[0:8], v[8:16], b[0:8], b[8:16]
        bs = bs + jnp.where(sub == 4, rolled(vs, 1, 0), 0.0)
        ps[c, t] = jnp.where(upper, rolled(bs, 4, 0), vs)
        bn = bn + jnp.where(sub == 3, rolled(vn, -1, 0), 0.0)
        pn[c, t] = jnp.where(upper, vn, rolled(bn, 4, 0))
        return v, b, x

    east = []
    for c in range(CH):
        v, b, _ = right_side(c, 0)
        pw[c] = jnp.where(low, v, rolled(b, L // 2, 1))
        v, b, x = right_side(c, TILES - 1)
        pe[c] = jnp.where(low, rolled(b, L // 2, 1), v)
        east.append(rolled(x, c + 1, 1))
    south_edge(0)
    south_edge(TILES - 1)
    sx[...] = jnp.where(lane == 0, east[0], jnp.where(lane == 1, east[1], east[2]))

    pl.semaphore_wait(barrier, len(peers))
    north8, south8 = pl.ds(0, 8), pl.ds(8, 8)
    e0 = [
        remote(pe, rw, 0, 1),
        remote(pw, re, 0, -1),
        remote(ps.at[:, TILES - 1], rn.at[:, TILES + 1], 1, 1),
        remote(ps.at[:, 0], rn.at[:, TILES], 1, -1),
        remote(pn.at[:, TILES - 1], rs.at[:, TILES + 1], -1, 1),
        remote(pn.at[:, 0], rs.at[:, TILES], -1, -1),
    ]
    edges = [
        remote(sx, wx, 0, 1),
        remote(sy.at[0], ey, 0, -1),
        remote(sy.at[TILES - 1], wy, 0, 1),
        remote(sy.at[0], ny.at[TILES], 1, -1),
        remote(sy.at[TILES - 1], ny.at[TILES + 1], 1, 1),
        remote(sx.at[north8], xsw, -1, 1),
        remote(sx.at[south8], xnw, 1, 1),
        remote(sx.at[north8], xs, -1, 0),
        remote(sx.at[south8], xn, 1, 0),
    ]
    for copy in e0 + edges:
        copy.start()

    for copy in loads[edge_loads:]:
        copy.wait()
    for t in range(1, TILES - 1):
        south_edge(t)
    to_south = remote(sy, ny.at[pl.ds(0, TILES)], 1, 0)
    to_south.start()
    edges.append(to_south)
    for c in range(CH):
        for t in range(1, TILES - 1):
            right_side(c, t)
    along = [
        remote(ps, rn.at[:, pl.ds(0, TILES)], 1, 0),
        remote(pn, rs.at[:, pl.ds(0, TILES)], -1, 0),
    ]
    for copy in along:
        copy.start()
    e0 += along

    inside0 = inside(0, -8, R0)
    has_north = jnp.where(lat > 0, 1.0, 0.0).astype(jnp.float32)
    for copy in edges:
        copy.wait()

    def column(x, c):
        return jnp.where(first if x.shape[0] == ROWS else first8, rolled(x, -c, 1), 0.0)

    def line(x, c):
        return jnp.where(sub == 0, x[c : c + 1], 0.0)

    for c in range(CH):
        b0[c, 0, own] = b0[c, 0, own] + column(wx[...], c)
        for t in range(TILES):
            b0[c, t, 8:16] = b0[c, t, 8:16] + has_north * line(ny[t], c)

    for copy in e0:
        copy.wait()

    for c in range(CH):
        halves = [(rn[c, t], rs[c, t]) for t in range(TILES)]
        halves.append(
            (jnp.where(low8, rn[c, TILES], rn[c, TILES + 1]), jnp.where(low8, rs[c, TILES], rs[c, TILES + 1]))
        )
        for t, (n, s) in enumerate(halves):
            v0[c, t, 0:8] = jnp.where(upper, 0.0, n) * inside0[0:8]
            v0[c, t, 24:32] = jnp.where(upper, s, 0.0) * inside0[24:32]
            n, s = rolled(n, 4, 0), rolled(s, 4, 0)
            below = sy[t] if t < TILES else jnp.where(low4, ey[...], wy[...])
            s = s + line(below, c)
            if t == 0:
                n, s = n + column(xnw[...], c), s + column(xsw[...], c)
            if t == TILES:
                n, s = n + column(xn[...], c), s + column(xs[...], c)
            b0[c, t, 0:8] = n
            b0[c, t, 24:32] = s
        v0[c, TILES, own] = jnp.where(low, re[c], rw[c])
        b = rolled(jnp.where(low, rw[c], re[c]), L // 2, 1) + column(sx[...], c)
        above = has_north * line(jnp.where(low4, ny[TILES], ny[TILES + 1]), c)
        b0[c, TILES, 8:16] = b[0:8] + above
        b0[c, TILES, 16:24] = b[8:16]

    for i in range(MAXS):
        a, b = (v0, w0) if i % 2 == 0 else (w0, v0)
        sweep(a, b, b0, T0, 4, 4, 24, inside0[4:28] * step(0, i), 1.0)

    restrict(v0, b0, b1, tmp, T0, O0, O0, ROWS, O1, 8, 1.0)
    for t in range(T1):
        rows = [b1[c, t, O1 : O1 + 8] for c in range(CH)]
        n, s = ([rolled(x, 2 * c + k, 0) for c, x in enumerate(rows)] for k in (0, 2))
        fn[t] = jnp.where(sub < 2, n[0], jnp.where(upper, n[1], n[2]))
        fs[t] = jnp.where(sub < 2, s[0], jnp.where(upper, s[1], s[2]))
    turned = [rolled(b1[c, T1 - 1, O1 : O1 + 8], WIDE + 2 * WIDE * c, 1) for c in range(CH)]
    hs[O1 : O1 + 8] = jnp.where(lane8 < 2 * WIDE, turned[0], jnp.where(lane8 < 4 * WIDE, turned[1], turned[2]))

    def sent(d):
        rows, there = pl.ds(O1, 8), pl.ds(O1 - 8 * d, 8)
        return [
            remote(b1.at[:, pl.ds(0, T1 - 1), rows], b1.at[:, pl.ds(0, T1 - 1), there], d, 0),
            remote(hs.at[rows], hs.at[there], d, 0),
        ]

    e1 = sent(2) + sent(-2)
    e1 += [remote(fs, gn, 3, 0), remote(fn, gs, -3, 0)]
    e1 += sent(1) + sent(-1)
    e2 = [
        remote(un, zs, -1, 0),
        remote(us, zn, 1, 0),
    ]
    for copy in e1:
        copy.start()
    for c in range(CH):
        for t in range(T0):
            un[c, t] = v0[c, t, O0 : O0 + 4]
            us[c, t] = v0[c, t, O0 + ROWS - 4 : O0 + ROWS]
    for copy in e2:
        copy.start()

    def factor(level, i, base, at, rows):
        return inside(level, at - base, rows) * step(level, i)

    for copy in e1:
        copy.wait()
    for c in range(CH):
        for t in range(T1):
            b1[c, t, 0:8] = rolled(gn[t], -2 * c - 2, 0)
            b1[c, t, 48:56] = rolled(gs[t], -2 * c, 0)
        for at, rows in ((8, 16), (32, 16)):
            b1[c, T1 - 1, at : at + rows] = rolled(hs[at : at + rows], -WIDE - 2 * WIDE * c, 1)

    f = factor(1, 0, O1, 0, R1)
    for c in range(CH):
        for t in range(T1):
            v1[c, t] = f * b1[c, t]
    sweep(v1, w1, b1, T1, 4, 4, 48, factor(1, 1, O1, 4, 48), 0.25)
    sweep(w1, v1, b1, T1, 8, 8, 40, factor(1, 2, O1, 8, 40), 0.25)
    sweep(v1, w1, b1, T1, 8, 8, 40, factor(1, 3, O1, 8, 40), 0.25)
    for c in range(CH):
        for t in range(T1):
            tmp[c, t, 40:48] = jnp.zeros((8, L), jnp.float32)
    restrict(w1, b1, b2, tmp, T1, 8, 8, 40, 0, R2, 0.25)

    f = factor(2, 0, O2, 0, R2)
    for c in range(CH):
        for t in range(T2):
            v2[c, t] = f * b2[c, t]
    for i in range(1, MAXS):
        a, b = (v2, w2) if i % 2 else (w2, v2)
        sweep(a, b, b2, T2, 2, 2, 16, factor(2, i, O2, 2, 16), 0.0625)

    insidep = inside(1, -OP, 24)
    for c in range(CH):
        prolong_rows(w2, c, T2, 4, 16, tmp)
        fine = prolong_cols([tmp[c, t, 0:24] for t in range(T2)], 24)
        for t in range(T1):
            vp[c, t, 0:24] = (w1[c, t, 16:40] + fine[t]) * insidep
    for i, (at, rows) in enumerate(((1, 24), (1, 24), (4, 16), (4, 16))):
        a, b = (vp, wp) if i % 2 == 0 else (wp, vp)
        sweep(a, b, b1, T1, at, at + O1 - OP, rows, factor(1, i, OP, at, rows), 0.25)

    for copy in e2:
        copy.wait()
    for c in range(CH):
        prolong_rows(vp, c, T1, 4, 16, tmp)
        fine = prolong_cols([tmp[c, t, 0:32] for t in range(T1)], 32)
        for t in range(T0):
            v0[c, t, 4:8] = (zn[c, t] + fine[t][4:8]) * inside0[4:8]
            v0[c, t, own] = v0[c, t, own] + fine[t][8:24]
            v0[c, t, 24:28] = (zs[c, t] + fine[t][24:28]) * inside0[24:28]
    for i in range(MAXS - 1):
        a, b = (v0, w0) if i % 2 == 0 else (w0, v0)
        sweep(a, b, b0, T0, 4, 4, 24, inside0[4:28] * step(0, i), 1.0)
    f = step(0, MAXS - 1)
    for c in range(CH):
        for t in range(TILES):
            x, r = residual(w0, b0, c, t, T0, O0, O0, ROWS, 1.0)
            out[c, :, t * L : (t + 1) * L] = x + f * r


def local(target, grad_x, grad_y, labels, sweeps):
    f32 = jnp.float32

    def vmem(*shape):
        return pltpu.VMEM(shape + (L,), f32)

    scratch = [
        pltpu.VMEM(grad_x.shape, f32),
        pltpu.VMEM(grad_y.shape, f32),
        pltpu.VMEM(labels.shape, jnp.int32),
        vmem(CH, T0, R0), vmem(CH, T0, R0), vmem(CH, T0, R0),
        vmem(TILES, 4), vmem(ROWS),
        vmem(TILES + 2, 4), vmem(4), vmem(4), vmem(ROWS),
        vmem(8), vmem(8), vmem(8), vmem(8),
        vmem(CH, TILES, 8), vmem(CH, TILES, 8),
        vmem(CH, TILES + 2, 8), vmem(CH, TILES + 2, 8),
        vmem(CH, ROWS), vmem(CH, ROWS), vmem(CH, ROWS), vmem(CH, ROWS),
        vmem(CH, T1, R1), vmem(CH, T1, R1), vmem(CH, T1, R1),
        vmem(CH, T1, RP), vmem(CH, T1, RP),
        vmem(CH, T2, R2), vmem(CH, T2, R2), vmem(CH, T2, R2),
        vmem(CH, T0, 4), vmem(CH, T0, 4), vmem(CH, T0, 4), vmem(CH, T0, 4),
        vmem(R1),
        vmem(T1, 8), vmem(T1, 8), vmem(T1, 8), vmem(T1, 8),
        vmem(CH, T0, 48),
        pltpu.SMEM((LEVELS,), jnp.int32),
        pltpu.SemaphoreType.DMA((18,)),
        pltpu.SemaphoreType.DMA((32,)),
        pltpu.SemaphoreType.DMA((32,)),
    ]
    anywhere = pl.BlockSpec(memory_space=pl.ANY)
    return pl.pallas_call(
        kernel,
        out_shape=pltpu.VMEM(target.shape, f32),
        in_specs=[anywhere] * 5,
        out_specs=pl.BlockSpec(memory_space=pltpu.VMEM),
        scratch_shapes=scratch,
        compiler_params=pltpu.CompilerParams(collective_id=0, has_side_effects=True),
        name="vcycle",
    )(sweeps, target, grad_x, grad_y, labels)


def solution(mesh):
    in_specs = (
        P(None, "lat", "lon"),
        P(None, None, "lat", "lon"),
        P(None, None, "lat", "lon"),
        P("lat", "lon"),
        P(),
    )
    out_specs = P(None, "lat", "lon")
    return jax.shard_map(local, mesh=mesh, in_specs=in_specs, out_specs=out_specs, check_vma=False)
```

```python
import jax
import jax.numpy as jnp
from jax import lax
from jax.experimental import pallas as pl
from jax.experimental.pallas import tpu as pltpu
from jax.sharding import PartitionSpec as P

SOURCES = 2
LEVELS = 3
MAXS = 4
CH = 3
ROWS = 16
TILES = 8
L = 128

screening = 0.02
damping = 0.8
MESH = pl.DeviceIdType.MESH

T0, T1, T2 = TILES + 1, TILES // 2 + 1, TILES // 4 + 1
O0, R0 = 8, 32
O1, R1 = 24, 56
OP, RP = 8, 32
O2, R2 = 8, 24
WIDE = 21


def iota(rows, dim):
    return lax.broadcasted_iota(jnp.int32, (rows, L), dim)


def lanes_of(rows):
    lane = iota(rows, 1)
    return lane == 0, lane == L - 1, lane < L // 2


def rolled(x, shift, dim):
    shift %= x.shape[dim]
    return pltpu.roll(x, shift, dim) if shift else x


def residual(src, rhs, c, t, tiles, at, rhs_at, rows, scale):
    diag = screening + 4.0 * scale
    first, last, _ = lanes_of(rows)
    x = src[c, t, at : at + rows]
    before = src[c, (t - 1) % tiles, at : at + rows]
    after = src[c, (t + 1) % tiles, at : at + rows]
    west = rolled(jnp.where(last, before, x), 1, 1)
    east = rolled(jnp.where(first, after, x), -1, 1)
    north = src[c, t, at - 1 : at - 1 + rows]
    south = src[c, t, at + 1 : at + 1 + rows]
    beside = (north + south) + (west + east)
    if scale != 1.0:
        beside = scale * beside
    return x, (rhs[c, t, rhs_at : rhs_at + rows] - diag * x) + beside


def sweep(src, dst, rhs, tiles, at, rhs_at, rows, factor, scale):
    for c in range(CH):
        for t in range(tiles):
            x, r = residual(src, rhs, c, t, tiles, at, rhs_at, rows, scale)
            dst[c, t, at : at + rows] = x + factor * r


def restrict(src, rhs, dst, tmp, tiles, at, rhs_at, rows, dst_at, count, scale, which):
    low = lanes_of(count)[2]
    pick = (2 * iota(count, 1)) % L
    for c in range(CH):
        parts = {}
        fine = [t for k in which for t in (2 * k, 2 * k + 1) if t < tiles]
        for t in fine:
            tmp[c, t, 0:rows] = residual(src, rhs, c, t, tiles, at, rhs_at, rows, scale)[1]
        for t in fine:
            pair = tmp[c, t, pl.ds(0, count, stride=2)] + tmp[c, t, pl.ds(1, count, stride=2)]
            pair = pair + rolled(pair, -1, 1)
            parts[t] = 0.25 * jnp.take_along_axis(pair, pick, axis=1)
        for k in which:
            x = parts[2 * k]
            if 2 * k + 1 < tiles:
                x = jnp.where(low, x, parts[2 * k + 1])
            dst[c, k, dst_at : dst_at + count] = x


def prolong_rows(src, c, tiles, at, rows, tmp):
    for t in range(tiles):
        x = 0.75 * src[c, t, at : at + rows]
        tmp[c, t, pl.ds(0, rows, stride=2)] = x + 0.25 * src[c, t, at - 1 : at - 1 + rows]
        tmp[c, t, pl.ds(1, rows, stride=2)] = x + 0.25 * src[c, t, at + 1 : at + 1 + rows]


def prolong_cols(xs, rows):
    lane = iota(rows, 1)
    first, last, low = lanes_of(rows)
    aside = jnp.where(lane % 2 == 0, L - 1, 1)
    count = len(xs)
    out = []
    for t in range(count):
        wests = rolled(xs[t - 1], 1, 1)
        easts = rolled(xs[(t + 1) % count], -1, 1)
        for h in range(2 if t < count - 1 else 1):
            here = lane // 2 + (h * (L // 2) if t < count - 1 else jnp.where(low, 0, L // 2))
            near = jnp.take_along_axis(xs[t], here, axis=1)
            far = jnp.take_along_axis(xs[t], (here + aside) % L, axis=1)
            if h == 0:
                far = jnp.where(first, wests, far)
            if h == 1 or t == count - 1:
                far = jnp.where(last, easts, far)
            out.append(0.75 * near + 0.25 * far)
    return out


def kernel(
    counts, target, grad_x, grad_y, labels, out,
    gx, gy, lab, v0, w0, b0, sy, sx, ny, ey, wy, wx, xn, xs, xnw, xsw,
    ps, pn, rn, rs, pe, pw, re, rw,
    vi, wi, b1, v1, w1, vp, wp, b2, v2, w2, zn, zs, un, us, hs, fn, fs, gn, gs, tmp,
    sweeps, in_sem, send, recv,
):
    lon, lat = lax.axis_index("lon"), lax.axis_index("lat")
    nlon, nlat = lax.axis_size("lon"), lax.axis_size("lat")

    def peer(dlat, dlon):
        return {"lat": lax.rem(lat + dlat + nlat, nlat), "lon": lax.rem(lon + dlon + nlon, nlon)}

    peers = [(d, 0) for d in (1, -1, 2, -2, 3, -3)]
    peers += [(i, j) for i in (-1, 0, 1) for j in (-1, 1)]
    barrier = pltpu.get_barrier_semaphore()
    for dlat, dlon in peers:
        pl.semaphore_signal(barrier, inc=1, device_id=peer(dlat, dlon), device_id_type=MESH)

    loads = []

    def load(src, dst):
        loads.append(pltpu.make_async_copy(src, dst, in_sem.at[len(loads)]))

    for tiles, cols in (((0,), pl.ds(0, L)), ((TILES - 1,), pl.ds((TILES - 2) * L, 2 * L))):
        load(grad_x.at[:, :, :, cols], gx.at[:, :, :, cols])
        load(grad_y.at[:, :, :, cols], gy.at[:, :, :, cols])
        load(labels.at[:, cols], lab.at[:, cols])
        for t in tiles:
            load(target.at[:, :, pl.ds(t * L, L)], v0.at[:, t, pl.ds(O0, ROWS)])
    edge_loads = len(loads)
    cols = pl.ds(L, (TILES - 3) * L)
    load(grad_x.at[:, :, :, cols], gx.at[:, :, :, cols])
    load(grad_y.at[:, :, :, cols], gy.at[:, :, :, cols])
    load(labels.at[:, cols], lab.at[:, cols])
    for t in range(1, TILES - 1):
        load(target.at[:, :, pl.ds(t * L, L)], v0.at[:, t, pl.ds(O0, ROWS)])
    load(counts, sweeps)
    for copy in loads:
        copy.start()

    used = [0]

    def remote(src, dst, dlat, dlon):
        k = used[0]
        used[0] += 1
        return pltpu.make_async_remote_copy(
            src_ref=src,
            dst_ref=dst,
            send_sem=send.at[k],
            recv_sem=recv.at[k],
            device_id=peer(dlat, dlon),
            device_id_type=MESH,
        )

    first, last, low = lanes_of(ROWS)
    first8, last8, low8 = lanes_of(8)
    low4 = lanes_of(4)[2]
    sub = iota(8, 0)
    lane, lane8 = iota(ROWS, 1), iota(8, 1)
    upper = sub < 4
    row = iota(ROWS, 0)

    def inside(level, start, rows):
        here = iota(rows, 0) + (start + lat * (ROWS >> level))
        return jnp.where((here >= 0) & (here < (nlat * ROWS >> level)), 1.0, 0.0).astype(jnp.float32)

    def step(level, i):
        full = damping / (screening + 4.0 * 0.25**level)
        return jnp.where(sweeps[level] > i, full, 0.0).astype(jnp.float32)

    for c in range(CH):
        for t in range(T0):
            for ref in (v0, w0):
                ref[c, t, 0:8] = jnp.zeros((8, L), jnp.float32)
                ref[c, t, 24:32] = jnp.zeros((8, L), jnp.float32)

    for copy in loads[:edge_loads]:
        copy.wait()

    def picked(ref, c, t, rows):
        cols = slice(t * L, (t + 1) * L)
        return jnp.where(lab[rows, cols] == 0, ref[0, c, rows, cols], ref[1, c, rows, cols])

    def south_edge(t):
        edge = [rolled(picked(gy, c, t, slice(8, 16)), c + 1, 0) for c in range(CH)]
        sy[t] = jnp.where(sub == 0, edge[0], jnp.where(sub == 1, edge[1], edge[2]))[0:4]

    own = slice(O0, O0 + ROWS)
    all_rows = slice(0, ROWS)

    def right_side(c, t):
        x = picked(gx, c, t, all_rows)
        y = picked(gy, c, t, all_rows)
        before = 0.0 if t == 0 else rolled(picked(gx, c, t - 1, all_rows), 1, 1)
        west = jnp.where(first, before, rolled(x, 1, 1))
        north = jnp.where(row == 0, 0.0, rolled(y, 1, 0))
        v = v0[c, t, own]
        b = screening * v - ((x - west) + (y - north))
        b0[c, t, own] = b
        vn, vs, bn, bs = v[0:8], v[8:16], b[0:8], b[8:16]
        bs = bs + jnp.where(sub == 4, rolled(vs, 1, 0), 0.0)
        ps[c, t] = jnp.where(upper, rolled(bs, 4, 0), vs)
        bn = bn + jnp.where(sub == 3, rolled(vn, -1, 0), 0.0)
        pn[c, t] = jnp.where(upper, vn, rolled(bn, 4, 0))
        return v, b, x

    east = []
    for c in range(CH):
        v, b, _ = right_side(c, 0)
        pw[c] = jnp.where(low, v, rolled(b, L // 2, 1))
        v, b, x = right_side(c, TILES - 1)
        pe[c] = jnp.where(low, rolled(b, L // 2, 1), v)
        east.append(rolled(x, c + 1, 1))
    south_edge(0)
    south_edge(TILES - 1)
    sx[...] = jnp.where(lane == 0, east[0], jnp.where(lane == 1, east[1], east[2]))

    pl.semaphore_wait(barrier, len(peers))
    north8, south8 = pl.ds(0, 8), pl.ds(8, 8)
    e0 = [
        remote(pe, rw, 0, 1),
        remote(pw, re, 0, -1),
        remote(ps.at[:, TILES - 1], rn.at[:, TILES + 1], 1, 1),
        remote(ps.at[:, 0], rn.at[:, TILES], 1, -1),
        remote(pn.at[:, TILES - 1], rs.at[:, TILES + 1], -1, 1),
        remote(pn.at[:, 0], rs.at[:, TILES], -1, -1),
    ]
    edges = [
        remote(sx, wx, 0, 1),
        remote(sy.at[0], ey, 0, -1),
        remote(sy.at[TILES - 1], wy, 0, 1),
        remote(sy.at[0], ny.at[TILES], 1, -1),
        remote(sy.at[TILES - 1], ny.at[TILES + 1], 1, 1),
        remote(sx.at[north8], xsw, -1, 1),
        remote(sx.at[south8], xnw, 1, 1),
        remote(sx.at[north8], xs, -1, 0),
        remote(sx.at[south8], xn, 1, 0),
    ]
    for copy in e0 + edges:
        copy.start()

    for copy in loads[edge_loads:]:
        copy.wait()
    for t in range(1, TILES - 1):
        south_edge(t)
    to_south = remote(sy, ny.at[pl.ds(0, TILES)], 1, 0)
    to_south.start()
    for c in range(CH):
        for t in range(1, TILES - 1):
            right_side(c, t)
    along = [
        remote(ps, rn.at[:, pl.ds(0, TILES)], 1, 0),
        remote(pn, rs.at[:, pl.ds(0, TILES)], -1, 0),
    ]
    for copy in along:
        copy.start()

    inside0 = inside(0, -8, R0)
    has_north = jnp.where(lat > 0, 1.0, 0.0).astype(jnp.float32)
    def column(x, c):
        return jnp.where(first if x.shape[0] == ROWS else first8, rolled(x, -c, 1), 0.0)

    def line(x, c):
        return jnp.where(sub == 0, x[c : c + 1], 0.0)

    for copy in along + [to_south]:
        copy.wait()
    for c in range(CH):
        for t in range(TILES):
            b0[c, t, 8:16] = b0[c, t, 8:16] + has_north * line(ny[t], c)
            n, s = rn[c, t], rs[c, t]
            v0[c, t, 0:8] = jnp.where(upper, 0.0, n) * inside0[0:8]
            v0[c, t, 24:32] = jnp.where(upper, s, 0.0) * inside0[24:32]
            b0[c, t, 0:8] = rolled(n, 4, 0)
            b0[c, t, 24:32] = rolled(s, 4, 0) + line(sy[t], c)

    f0 = [inside0[4:28] * step(0, i) for i in range(MAXS)]
    inner = (1, 2)
    for i in range(MAXS):
        a, b = ((v0, wi), (wi, vi), (vi, wi), (wi, vi))[i]
        sweep(a, b, b0, TILES, 4, 4, 24, f0[i], 1.0)
    restrict(vi, b0, b1, tmp, TILES, O0, O0, ROWS, O1, 8, 1.0, inner)
    rows1 = pl.ds(O1, 8)

    def there(d):
        return pl.ds(O1 - 8 * d, 8)

    e1 = [
        remote(b1.at[:, pl.ds(1, 2), rows1], b1.at[:, pl.ds(1, 2), there(d)], d, 0) for d in (2, -2, 1, -1)
    ]
    for copy in e1:
        copy.start()

    for copy in edges + e0:
        copy.wait()
    for c in range(CH):
        b0[c, 0, own] = b0[c, 0, own] + column(wx[...], c)
        b0[c, 0, 0:8] = b0[c, 0, 0:8] + column(xnw[...], c)
        b0[c, 0, 24:32] = b0[c, 0, 24:32] + column(xsw[...], c)
        n = jnp.where(low8, rn[c, TILES], rn[c, TILES + 1])
        s = jnp.where(low8, rs[c, TILES], rs[c, TILES + 1])
        v0[c, TILES, 0:8] = jnp.where(upper, 0.0, n) * inside0[0:8]
        v0[c, TILES, 24:32] = jnp.where(upper, s, 0.0) * inside0[24:32]
        s = rolled(s, 4, 0) + line(jnp.where(low4, ey[...], wy[...]), c)
        b0[c, TILES, 0:8] = rolled(n, 4, 0) + column(xn[...], c)
        b0[c, TILES, 24:32] = s + column(xs[...], c)
        v0[c, TILES, own] = jnp.where(low, re[c], rw[c])
        b = rolled(jnp.where(low, rw[c], re[c]), L // 2, 1) + column(sx[...], c)
        above = has_north * line(jnp.where(low4, ny[TILES], ny[TILES + 1]), c)
        b0[c, TILES, 8:16] = b[0:8] + above
        b0[c, TILES, 16:24] = b[8:16]

    for i in range(MAXS):
        a, b = (v0, w0) if i % 2 == 0 else (w0, v0)
        sweep(a, b, b0, T0, 4, 4, 24, f0[i], 1.0)

    restrict(v0, b0, b1, tmp, T0, O0, O0, ROWS, O1, 8, 1.0, (0, 3, 4))
    for t in range(T1):
        rows = [b1[c, t, O1 : O1 + 8] for c in range(CH)]
        n, s = ([rolled(x, 2 * c + k, 0) for c, x in enumerate(rows)] for k in (0, 2))
        fn[t] = jnp.where(sub < 2, n[0], jnp.where(upper, n[1], n[2]))
        fs[t] = jnp.where(sub < 2, s[0], jnp.where(upper, s[1], s[2]))
    turned = [rolled(b1[c, T1 - 1, O1 : O1 + 8], WIDE + 2 * WIDE * c, 1) for c in range(CH)]
    hs[O1 : O1 + 8] = jnp.where(lane8 < 2 * WIDE, turned[0], jnp.where(lane8 < 4 * WIDE, turned[1], turned[2]))

    def sent(d):
        return [
            remote(b1.at[:, 0, rows1], b1.at[:, 0, there(d)], d, 0),
            remote(b1.at[:, 3, rows1], b1.at[:, 3, there(d)], d, 0),
            remote(hs.at[rows1], hs.at[there(d)], d, 0),
        ]

    late = sent(2) + sent(-2)
    late += [remote(fs, gn, 3, 0), remote(fn, gs, -3, 0)]
    late += sent(1) + sent(-1)
    e2 = [
        remote(un, zs, -1, 0),
        remote(us, zn, 1, 0),
    ]
    for copy in late:
        copy.start()
    e1 += late
    for c in range(CH):
        for t in range(T0):
            un[c, t] = v0[c, t, O0 : O0 + 4]
            us[c, t] = v0[c, t, O0 + ROWS - 4 : O0 + ROWS]
    for copy in e2:
        copy.start()

    def factor(level, i, base, at, rows):
        return inside(level, at - base, rows) * step(level, i)

    for copy in e1:
        copy.wait()
    for c in range(CH):
        for t in range(T1):
            b1[c, t, 0:8] = rolled(gn[t], -2 * c - 2, 0)
            b1[c, t, 48:56] = rolled(gs[t], -2 * c, 0)
        for at, rows in ((8, 16), (32, 16)):
            b1[c, T1 - 1, at : at + rows] = rolled(hs[at : at + rows], -WIDE - 2 * WIDE * c, 1)

    f = factor(1, 0, O1, 0, R1)
    for c in range(CH):
        for t in range(T1):
            v1[c, t] = f * b1[c, t]
    sweep(v1, w1, b1, T1, 4, 4, 48, factor(1, 1, O1, 4, 48), 0.25)
    sweep(w1, v1, b1, T1, 8, 8, 40, factor(1, 2, O1, 8, 40), 0.25)
    sweep(v1, w1, b1, T1, 8, 8, 40, factor(1, 3, O1, 8, 40), 0.25)
    for c in range(CH):
        for t in range(T1):
            tmp[c, t, 40:48] = jnp.zeros((8, L), jnp.float32)
    restrict(w1, b1, b2, tmp, T1, 8, 8, 40, 0, R2, 0.25, range(T2))

    f = factor(2, 0, O2, 0, R2)
    for c in range(CH):
        for t in range(T2):
            v2[c, t] = f * b2[c, t]
    for i in range(1, MAXS):
        a, b = (v2, w2) if i % 2 else (w2, v2)
        sweep(a, b, b2, T2, 2, 2, 16, factor(2, i, O2, 2, 16), 0.0625)

    insidep = inside(1, -OP, 24)
    for c in range(CH):
        prolong_rows(w2, c, T2, 4, 16, tmp)
        fine = prolong_cols([tmp[c, t, 0:24] for t in range(T2)], 24)
        for t in range(T1):
            vp[c, t, 0:24] = (w1[c, t, 16:40] + fine[t]) * insidep
    for i, (at, rows) in enumerate(((1, 24), (1, 24), (4, 16), (4, 16))):
        a, b = (vp, wp) if i % 2 == 0 else (wp, vp)
        sweep(a, b, b1, T1, at, at + O1 - OP, rows, factor(1, i, OP, at, rows), 0.25)

    for copy in e2:
        copy.wait()
    for c in range(CH):
        prolong_rows(vp, c, T1, 4, 16, tmp)
        fine = prolong_cols([tmp[c, t, 0:32] for t in range(T1)], 32)
        for t in range(T0):
            v0[c, t, 4:8] = (zn[c, t] + fine[t][4:8]) * inside0[4:8]
            v0[c, t, own] = v0[c, t, own] + fine[t][8:24]
            v0[c, t, 24:28] = (zs[c, t] + fine[t][24:28]) * inside0[24:28]
    for i in range(MAXS - 1):
        a, b = (v0, w0) if i % 2 == 0 else (w0, v0)
        sweep(a, b, b0, T0, 4, 4, 24, f0[i], 1.0)
    f = step(0, MAXS - 1)
    for c in range(CH):
        for t in range(TILES):
            x, r = residual(w0, b0, c, t, T0, O0, O0, ROWS, 1.0)
            out[c, :, t * L : (t + 1) * L] = x + f * r


def local(target, grad_x, grad_y, labels, sweeps):
    f32 = jnp.float32

    def vmem(*shape):
        return pltpu.VMEM(shape + (L,), f32)

    scratch = [
        pltpu.VMEM(grad_x.shape, f32),
        pltpu.VMEM(grad_y.shape, f32),
        pltpu.VMEM(labels.shape, jnp.int32),
        vmem(CH, T0, R0), vmem(CH, T0, R0), vmem(CH, T0, R0),
        vmem(TILES, 4), vmem(ROWS),
        vmem(TILES + 2, 4), vmem(4), vmem(4), vmem(ROWS),
        vmem(8), vmem(8), vmem(8), vmem(8),
        vmem(CH, TILES, 8), vmem(CH, TILES, 8),
        vmem(CH, TILES + 2, 8), vmem(CH, TILES + 2, 8),
        vmem(CH, ROWS), vmem(CH, ROWS), vmem(CH, ROWS), vmem(CH, ROWS),
        vmem(CH, TILES, R0), vmem(CH, TILES, R0),
        vmem(CH, T1, R1), vmem(CH, T1, R1), vmem(CH, T1, R1),
        vmem(CH, T1, RP), vmem(CH, T1, RP),
        vmem(CH, T2, R2), vmem(CH, T2, R2), vmem(CH, T2, R2),
        vmem(CH, T0, 4), vmem(CH, T0, 4), vmem(CH, T0, 4), vmem(CH, T0, 4),
        vmem(R1),
        vmem(T1, 8), vmem(T1, 8), vmem(T1, 8), vmem(T1, 8),
        vmem(CH, T0, 48),
        pltpu.SMEM((LEVELS,), jnp.int32),
        pltpu.SemaphoreType.DMA((18,)),
        pltpu.SemaphoreType.DMA((40,)),
        pltpu.SemaphoreType.DMA((40,)),
    ]
    anywhere = pl.BlockSpec(memory_space=pl.ANY)
    return pl.pallas_call(
        kernel,
        out_shape=pltpu.VMEM(target.shape, f32),
        in_specs=[anywhere] * 5,
        out_specs=pl.BlockSpec(memory_space=pltpu.VMEM),
        scratch_shapes=scratch,
        compiler_params=pltpu.CompilerParams(collective_id=0, has_side_effects=True),
        name="vcycle",
    )(sweeps, target, grad_x, grad_y, labels)


def solution(mesh):
    in_specs = (
        P(None, "lat", "lon"),
        P(None, None, "lat", "lon"),
        P(None, None, "lat", "lon"),
        P("lat", "lon"),
        P(),
    )
    out_specs = P(None, "lat", "lon")
    return jax.shard_map(local, mesh=mesh, in_specs=in_specs, out_specs=out_specs, check_vma=False)
```

```python
import jax
import jax.numpy as jnp
from jax import lax
from jax.experimental import pallas as pl
from jax.experimental.pallas import tpu as pltpu
from jax.sharding import PartitionSpec as P

SOURCES = 2
LEVELS = 3
MAXS = 4
CH = 3
ROWS = 16
TILES = 8
L = 128

screening = 0.02
damping = 0.8
MESH = pl.DeviceIdType.MESH

T0, T1, T2 = TILES + 1, TILES // 2 + 1, TILES // 4 + 1
O0, R0 = 8, 32
O1, R1 = 24, 56
OP, RP = 8, 32
O2, R2 = 8, 24
WIDE = 21


def iota(rows, dim):
    return lax.broadcasted_iota(jnp.int32, (rows, L), dim)


def lanes_of(rows):
    lane = iota(rows, 1)
    return lane == 0, lane == L - 1, lane < L // 2


def rolled(x, shift, dim):
    shift %= x.shape[dim]
    return pltpu.roll(x, shift, dim) if shift else x


def residual(src, rhs, c, t, tiles, at, rhs_at, rows, scale):
    diag = screening + 4.0 * scale
    first, last, _ = lanes_of(rows)
    x = src[c, t, at : at + rows]
    before = src[c, (t - 1) % tiles, at : at + rows]
    after = src[c, (t + 1) % tiles, at : at + rows]
    west = rolled(jnp.where(last, before, x), 1, 1)
    east = rolled(jnp.where(first, after, x), -1, 1)
    north = src[c, t, at - 1 : at - 1 + rows]
    south = src[c, t, at + 1 : at + 1 + rows]
    beside = (north + south) + (west + east)
    if scale != 1.0:
        beside = scale * beside
    return x, (rhs[c, t, rhs_at : rhs_at + rows] - diag * x) + beside


def sweep(src, dst, rhs, tiles, at, rhs_at, rows, factor, scale):
    for c in range(CH):
        for t in range(tiles):
            x, r = residual(src, rhs, c, t, tiles, at, rhs_at, rows, scale)
            dst[c, t, at : at + rows] = x + factor * r


def restrict(src, rhs, dst, tmp, tiles, at, rhs_at, rows, dst_at, count, scale, which):
    low = lanes_of(count)[2]
    pick = (2 * iota(count, 1)) % L
    for c in range(CH):
        parts = {}
        fine = [t for k in which for t in (2 * k, 2 * k + 1) if t < tiles]
        for t in fine:
            tmp[c, t, 0:rows] = residual(src, rhs, c, t, tiles, at, rhs_at, rows, scale)[1]
        for t in fine:
            pair = tmp[c, t, pl.ds(0, count, stride=2)] + tmp[c, t, pl.ds(1, count, stride=2)]
            pair = pair + rolled(pair, -1, 1)
            parts[t] = 0.25 * jnp.take_along_axis(pair, pick, axis=1)
        for k in which:
            x = parts[2 * k]
            if 2 * k + 1 < tiles:
                x = jnp.where(low, x, parts[2 * k + 1])
            dst[c, k, dst_at : dst_at + count] = x


def prolong_rows(src, c, tiles, at, rows, tmp):
    for t in range(tiles):
        x = 0.75 * src[c, t, at : at + rows]
        tmp[c, t, pl.ds(0, rows, stride=2)] = x + 0.25 * src[c, t, at - 1 : at - 1 + rows]
        tmp[c, t, pl.ds(1, rows, stride=2)] = x + 0.25 * src[c, t, at + 1 : at + 1 + rows]


def prolong_cols(xs, rows):
    lane = iota(rows, 1)
    first, last, low = lanes_of(rows)
    aside = jnp.where(lane % 2 == 0, L - 1, 1)
    count = len(xs)
    out = []
    for t in range(count):
        wests = rolled(xs[t - 1], 1, 1)
        easts = rolled(xs[(t + 1) % count], -1, 1)
        for h in range(2 if t < count - 1 else 1):
            here = lane // 2 + (h * (L // 2) if t < count - 1 else jnp.where(low, 0, L // 2))
            near = jnp.take_along_axis(xs[t], here, axis=1)
            far = jnp.take_along_axis(xs[t], (here + aside) % L, axis=1)
            if h == 0:
                far = jnp.where(first, wests, far)
            if h == 1 or t == count - 1:
                far = jnp.where(last, easts, far)
            out.append(0.75 * near + 0.25 * far)
    return out


def kernel(
    counts, target, grad_x, grad_y, labels, out,
    gx, gy, lab, v0, w0, b0, sy, sx, ny, ey, wy, wx, xn, xs, xnw, xsw,
    ps, pn, rn, rs, pe, pw, re, rw,
    vi, wi, b1, v1, w1, vp, wp, b2, v2, w2, zn, zs, un, us, hs, fn, fs, gn, gs, tmp,
    sweeps, in_sem, send, recv,
):
    lon, lat = lax.axis_index("lon"), lax.axis_index("lat")
    nlon, nlat = lax.axis_size("lon"), lax.axis_size("lat")

    def peer(dlat, dlon):
        return {"lat": lax.rem(lat + dlat + nlat, nlat), "lon": lax.rem(lon + dlon + nlon, nlon)}

    peers = [(d, 0) for d in (1, -1, 2, -2, 3, -3)]
    peers += [(i, j) for i in (-1, 0, 1) for j in (-1, 1)]
    barrier = pltpu.get_barrier_semaphore()
    for dlat, dlon in peers:
        pl.semaphore_signal(barrier, inc=1, device_id=peer(dlat, dlon), device_id_type=MESH)

    loads = []

    def load(src, dst):
        loads.append(pltpu.make_async_copy(src, dst, in_sem.at[len(loads)]))

    for tiles, cols in (((0,), pl.ds(0, L)), ((TILES - 1,), pl.ds((TILES - 2) * L, 2 * L))):
        load(grad_x.at[:, :, :, cols], gx.at[:, :, :, cols])
        load(grad_y.at[:, :, :, cols], gy.at[:, :, :, cols])
        load(labels.at[:, cols], lab.at[:, cols])
        for t in tiles:
            load(target.at[:, :, pl.ds(t * L, L)], v0.at[:, t, pl.ds(O0, ROWS)])
    edge_loads = len(loads)
    cols = pl.ds(L, (TILES - 3) * L)
    load(grad_x.at[:, :, :, cols], gx.at[:, :, :, cols])
    load(grad_y.at[:, :, :, cols], gy.at[:, :, :, cols])
    load(labels.at[:, cols], lab.at[:, cols])
    for t in range(1, TILES - 1):
        load(target.at[:, :, pl.ds(t * L, L)], v0.at[:, t, pl.ds(O0, ROWS)])
    load(counts, sweeps)
    for copy in loads:
        copy.start()

    used = [0]

    def remote(src, dst, dlat, dlon):
        k = used[0]
        used[0] += 1
        return pltpu.make_async_remote_copy(
            src_ref=src,
            dst_ref=dst,
            send_sem=send.at[k],
            recv_sem=recv.at[k],
            device_id=peer(dlat, dlon),
            device_id_type=MESH,
        )

    first, last, low = lanes_of(ROWS)
    first8, last8, low8 = lanes_of(8)
    low4 = lanes_of(4)[2]
    sub = iota(8, 0)
    lane, lane8 = iota(ROWS, 1), iota(8, 1)
    upper = sub < 4
    row = iota(ROWS, 0)

    def inside(level, start, rows):
        here = iota(rows, 0) + (start + lat * (ROWS >> level))
        return jnp.where((here >= 0) & (here < (nlat * ROWS >> level)), 1.0, 0.0).astype(jnp.float32)

    def step(level, i):
        full = damping / (screening + 4.0 * 0.25**level)
        return jnp.where(sweeps[level] > i, full, 0.0).astype(jnp.float32)

    for c in range(CH):
        for t in range(T0):
            for ref in (v0, w0):
                ref[c, t, 0:8] = jnp.zeros((8, L), jnp.float32)
                ref[c, t, 24:32] = jnp.zeros((8, L), jnp.float32)

    for copy in loads[:edge_loads]:
        copy.wait()

    def picked(ref, c, t, rows):
        cols = slice(t * L, (t + 1) * L)
        return jnp.where(lab[rows, cols] == 0, ref[0, c, rows, cols], ref[1, c, rows, cols])

    def south_edge(t):
        edge = [rolled(picked(gy, c, t, slice(8, 16)), c + 1, 0) for c in range(CH)]
        sy[t] = jnp.where(sub == 0, edge[0], jnp.where(sub == 1, edge[1], edge[2]))[0:4]

    own = slice(O0, O0 + ROWS)
    all_rows = slice(0, ROWS)

    def right_side(c, t):
        x = picked(gx, c, t, all_rows)
        y = picked(gy, c, t, all_rows)
        before = 0.0 if t == 0 else rolled(picked(gx, c, t - 1, all_rows), 1, 1)
        west = jnp.where(first, before, rolled(x, 1, 1))
        north = jnp.where(row == 0, 0.0, rolled(y, 1, 0))
        v = v0[c, t, own]
        b = screening * v - ((x - west) + (y - north))
        b0[c, t, own] = b
        vn, vs, bn, bs = v[0:8], v[8:16], b[0:8], b[8:16]
        bs = bs + jnp.where(sub == 4, rolled(vs, 1, 0), 0.0)
        ps[c, t] = jnp.where(upper, rolled(bs, 4, 0), vs)
        bn = bn + jnp.where(sub == 3, rolled(vn, -1, 0), 0.0)
        pn[c, t] = jnp.where(upper, vn, rolled(bn, 4, 0))
        return v, b, x

    east = []
    for c in range(CH):
        v, b, _ = right_side(c, 0)
        pw[c] = jnp.where(low, v, rolled(b, L // 2, 1))
        v, b, x = right_side(c, TILES - 1)
        pe[c] = jnp.where(low, rolled(b, L // 2, 1), v)
        east.append(rolled(x, c + 1, 1))
    south_edge(0)
    south_edge(TILES - 1)
    sx[...] = jnp.where(lane == 0, east[0], jnp.where(lane == 1, east[1], east[2]))

    pl.semaphore_wait(barrier, len(peers))
    north8, south8 = pl.ds(0, 8), pl.ds(8, 8)
    e0 = [
        remote(pe, rw, 0, 1),
        remote(pw, re, 0, -1),
        remote(ps.at[:, TILES - 1], rn.at[:, TILES + 1], 1, 1),
        remote(ps.at[:, 0], rn.at[:, TILES], 1, -1),
        remote(pn.at[:, TILES - 1], rs.at[:, TILES + 1], -1, 1),
        remote(pn.at[:, 0], rs.at[:, TILES], -1, -1),
    ]
    edges = [
        remote(sx, wx, 0, 1),
        remote(sy.at[0], ey, 0, -1),
        remote(sy.at[TILES - 1], wy, 0, 1),
        remote(sy.at[0], ny.at[TILES], 1, -1),
        remote(sy.at[TILES - 1], ny.at[TILES + 1], 1, 1),
        remote(sx.at[north8], xsw, -1, 1),
        remote(sx.at[south8], xnw, 1, 1),
        remote(sx.at[north8], xs, -1, 0),
        remote(sx.at[south8], xn, 1, 0),
    ]
    for copy in e0 + edges:
        copy.start()

    for copy in loads[edge_loads:]:
        copy.wait()
    for t in range(1, TILES - 1):
        south_edge(t)
    to_south = remote(sy, ny.at[pl.ds(0, TILES)], 1, 0)
    to_south.start()
    for c in range(CH):
        for t in range(1, TILES - 1):
            right_side(c, t)
    along = [
        remote(ps, rn.at[:, pl.ds(0, TILES)], 1, 0),
        remote(pn, rs.at[:, pl.ds(0, TILES)], -1, 0),
    ]
    for copy in along:
        copy.start()

    inside0 = inside(0, -8, R0)
    has_north = jnp.where(lat > 0, 1.0, 0.0).astype(jnp.float32)
    def column(x, c):
        return jnp.where(first if x.shape[0] == ROWS else first8, rolled(x, -c, 1), 0.0)

    def line(x, c):
        return jnp.where(sub == 0, x[c : c + 1], 0.0)

    for copy in along + [to_south]:
        copy.wait()
    for c in range(CH):
        for t in range(TILES):
            b0[c, t, 8:16] = b0[c, t, 8:16] + has_north * line(ny[t], c)
            n, s = rn[c, t], rs[c, t]
            v0[c, t, 0:8] = jnp.where(upper, 0.0, n) * inside0[0:8]
            v0[c, t, 24:32] = jnp.where(upper, s, 0.0) * inside0[24:32]
            b0[c, t, 0:8] = rolled(n, 4, 0)
            b0[c, t, 24:32] = rolled(s, 4, 0) + line(sy[t], c)

    f0 = [inside0[4:28] * step(0, i) for i in range(MAXS)]
    inner = (1, 2)
    for i in range(MAXS):
        a, b = ((v0, wi), (wi, vi), (vi, wi), (wi, vi))[i]
        sweep(a, b, b0, TILES, 4, 4, 24, f0[i], 1.0)
    restrict(vi, b0, b1, tmp, TILES, O0, O0, ROWS, O1, 8, 1.0, inner)
    rows1 = pl.ds(O1, 8)

    def there(d):
        return pl.ds(O1 - 8 * d, 8)

    e1 = [
        remote(b1.at[:, pl.ds(1, 2), rows1], b1.at[:, pl.ds(1, 2), there(d)], d, 0) for d in (2, -2, 1, -1)
    ]
    for copy in e1:
        copy.start()

    for copy in edges + e0:
        copy.wait()
    for c in range(CH):
        b0[c, 0, own] = b0[c, 0, own] + column(wx[...], c)
        b0[c, 0, 0:8] = b0[c, 0, 0:8] + column(xnw[...], c)
        b0[c, 0, 24:32] = b0[c, 0, 24:32] + column(xsw[...], c)
        n = jnp.where(low8, rn[c, TILES], rn[c, TILES + 1])
        s = jnp.where(low8, rs[c, TILES], rs[c, TILES + 1])
        v0[c, TILES, 0:8] = jnp.where(upper, 0.0, n) * inside0[0:8]
        v0[c, TILES, 24:32] = jnp.where(upper, s, 0.0) * inside0[24:32]
        s = rolled(s, 4, 0) + line(jnp.where(low4, ey[...], wy[...]), c)
        b0[c, TILES, 0:8] = rolled(n, 4, 0) + column(xn[...], c)
        b0[c, TILES, 24:32] = s + column(xs[...], c)
        v0[c, TILES, own] = jnp.where(low, re[c], rw[c])
        b = rolled(jnp.where(low, rw[c], re[c]), L // 2, 1) + column(sx[...], c)
        above = has_north * line(jnp.where(low4, ny[TILES], ny[TILES + 1]), c)
        b0[c, TILES, 8:16] = b[0:8] + above
        b0[c, TILES, 16:24] = b[8:16]

    for i in range(MAXS):
        a, b = (v0, w0) if i % 2 == 0 else (w0, v0)
        sweep(a, b, b0, T0, 4, 4, 24, f0[i], 1.0)

    restrict(v0, b0, b1, tmp, T0, O0, O0, ROWS, O1, 8, 1.0, (0, 3, 4))
    for t in range(T1):
        rows = [b1[c, t, O1 : O1 + 8] for c in range(CH)]
        n, s = ([rolled(x, 2 * c + k, 0) for c, x in enumerate(rows)] for k in (0, 2))
        fn[t] = jnp.where(sub < 2, n[0], jnp.where(upper, n[1], n[2]))
        fs[t] = jnp.where(sub < 2, s[0], jnp.where(upper, s[1], s[2]))
    turned = [rolled(b1[c, T1 - 1, O1 : O1 + 8], WIDE + 2 * WIDE * c, 1) for c in range(CH)]
    hs[O1 : O1 + 8] = jnp.where(lane8 < 2 * WIDE, turned[0], jnp.where(lane8 < 4 * WIDE, turned[1], turned[2]))

    def sent(d):
        return [
            remote(b1.at[:, 0, rows1], b1.at[:, 0, there(d)], d, 0),
            remote(b1.at[:, 3, rows1], b1.at[:, 3, there(d)], d, 0),
            remote(hs.at[rows1], hs.at[there(d)], d, 0),
        ]

    late = sent(2) + sent(-2)
    late += [remote(fs, gn, 3, 0), remote(fn, gs, -3, 0)]
    late += sent(1) + sent(-1)
    e2 = [
        remote(un, zs, -1, 0),
        remote(us, zn, 1, 0),
    ]
    for copy in late:
        copy.start()
    e1 += late
    for c in range(CH):
        for t in range(T0):
            un[c, t] = v0[c, t, O0 : O0 + 4]
            us[c, t] = v0[c, t, O0 + ROWS - 4 : O0 + ROWS]
    for copy in e2:
        copy.start()

    def factor(level, i, base, at, rows):
        return inside(level, at - base, rows) * step(level, i)

    for copy in e1:
        copy.wait()
    for c in range(CH):
        for t in range(T1):
            b1[c, t, 0:8] = rolled(gn[t], -2 * c - 2, 0)
            b1[c, t, 48:56] = rolled(gs[t], -2 * c, 0)
        for at, rows in ((8, 16), (32, 16)):
            b1[c, T1 - 1, at : at + rows] = rolled(hs[at : at + rows], -WIDE - 2 * WIDE * c, 1)

    f = factor(1, 0, O1, 0, R1)
    for c in range(CH):
        for t in range(T1):
            v1[c, t] = f * b1[c, t]
    sweep(v1, w1, b1, T1, 4, 4, 48, factor(1, 1, O1, 4, 48), 0.25)
    sweep(w1, v1, b1, T1, 8, 8, 40, factor(1, 2, O1, 8, 40), 0.25)
    sweep(v1, w1, b1, T1, 8, 8, 40, factor(1, 3, O1, 8, 40), 0.25)
    for c in range(CH):
        for t in range(T1):
            tmp[c, t, 40:48] = jnp.zeros((8, L), jnp.float32)
    restrict(w1, b1, b2, tmp, T1, 8, 8, 40, 0, R2, 0.25, range(T2))

    f = factor(2, 0, O2, 0, R2)
    for c in range(CH):
        for t in range(T2):
            v2[c, t] = f * b2[c, t]
    for i in range(1, MAXS):
        a, b = (v2, w2) if i % 2 else (w2, v2)
        sweep(a, b, b2, T2, 2, 2, 16, factor(2, i, O2, 2, 16), 0.0625)

    insidep = inside(1, -OP, 24)
    for c in range(CH):
        prolong_rows(w2, c, T2, 4, 16, tmp)
        fine = prolong_cols([tmp[c, t, 0:24] for t in range(T2)], 24)
        for t in range(T1):
            vp[c, t, 0:24] = (w1[c, t, 16:40] + fine[t]) * insidep
    for i, (at, rows) in enumerate(((1, 24), (1, 24), (4, 16), (4, 16))):
        a, b = (vp, wp) if i % 2 == 0 else (wp, vp)
        sweep(a, b, b1, T1, at, at + O1 - OP, rows, factor(1, i, OP, at, rows), 0.25)

    for copy in e2:
        copy.wait()
    for c in range(CH):
        prolong_rows(vp, c, T1, 4, 16, tmp)
        fine = prolong_cols([tmp[c, t, 0:32] for t in range(T1)], 32)
        for t in range(T0):
            v0[c, t, 4:8] = (zn[c, t] + fine[t][4:8]) * inside0[4:8]
            v0[c, t, own] = v0[c, t, own] + fine[t][8:24]
            v0[c, t, 24:28] = (zs[c, t] + fine[t][24:28]) * inside0[24:28]
    for i in range(MAXS - 1):
        a, b = (v0, w0) if i % 2 == 0 else (w0, v0)
        sweep(a, b, b0, T0, 4, 4, 24, f0[i], 1.0)
    f = step(0, MAXS - 1)
    for c in range(CH):
        for t in range(TILES):
            x, r = residual(w0, b0, c, t, T0, O0, O0, ROWS, 1.0)
            out[c, :, t * L : (t + 1) * L] = x + f * r


def local(target, grad_x, grad_y, labels, sweeps):
    f32 = jnp.float32

    def vmem(*shape):
        return pltpu.VMEM(shape + (L,), f32)

    scratch = [
        pltpu.VMEM(grad_x.shape, f32),
        pltpu.VMEM(grad_y.shape, f32),
        pltpu.VMEM(labels.shape, jnp.int32),
        vmem(CH, T0, R0), vmem(CH, T0, R0), vmem(CH, T0, R0),
        vmem(TILES, 4), vmem(ROWS),
        vmem(TILES + 2, 4), vmem(4), vmem(4), vmem(ROWS),
        vmem(8), vmem(8), vmem(8), vmem(8),
        vmem(CH, TILES, 8), vmem(CH, TILES, 8),
        vmem(CH, TILES + 2, 8), vmem(CH, TILES + 2, 8),
        vmem(CH, ROWS), vmem(CH, ROWS), vmem(CH, ROWS), vmem(CH, ROWS),
        vmem(CH, TILES, R0), vmem(CH, TILES, R0),
        vmem(CH, T1, R1), vmem(CH, T1, R1), vmem(CH, T1, R1),
        vmem(CH, T1, RP), vmem(CH, T1, RP),
        vmem(CH, T2, R2), vmem(CH, T2, R2), vmem(CH, T2, R2),
        vmem(CH, T0, 4), vmem(CH, T0, 4), vmem(CH, T0, 4), vmem(CH, T0, 4),
        vmem(R1),
        vmem(T1, 8), vmem(T1, 8), vmem(T1, 8), vmem(T1, 8),
        vmem(CH, T0, 56),
        pltpu.SMEM((LEVELS,), jnp.int32),
        pltpu.SemaphoreType.DMA((18,)),
        pltpu.SemaphoreType.DMA((40,)),
        pltpu.SemaphoreType.DMA((40,)),
    ]
    anywhere = pl.BlockSpec(memory_space=pl.ANY)
    return pl.pallas_call(
        kernel,
        out_shape=pltpu.VMEM(target.shape, f32),
        in_specs=[anywhere] * 5,
        out_specs=pl.BlockSpec(memory_space=pltpu.VMEM),
        scratch_shapes=scratch,
        compiler_params=pltpu.CompilerParams(collective_id=0, has_side_effects=True),
        name="vcycle",
    )(sweeps, target, grad_x, grad_y, labels)


def solution(mesh):
    in_specs = (
        P(None, "lat", "lon"),
        P(None, None, "lat", "lon"),
        P(None, None, "lat", "lon"),
        P("lat", "lon"),
        P(),
    )
    out_specs = P(None, "lat", "lon")
    return jax.shard_map(local, mesh=mesh, in_specs=in_specs, out_specs=out_specs, check_vma=False)
```
